256 devices in a mesh: gx: 16 (over z_hi, y), gy: 16 (over z_lo, x, core).
Axes of the slice: x: 4, y: 4, z: 8 (z_hi: 4, z_lo: 2; z = z_hi * 2 + z_lo), core: 2. Of those that a mesh axis runs over, the one named last changes fastest.
Arguments:
- goal_embed: bfloat16 [32768, 128], P(('gx', 'gy')), may hold values from -6 to 6
- goal_bins: int32 [32768], P(('gx', 'gy')), may hold values from 0 to 16383, as said below
- goal_weights: float32 [32768], P(('gx', 'gy')), may hold values from 0.1 to 10
Outputs:
- bin_mean: float32 [16384, 128], P(('gx', 'gy'))
- rarity: float32 [16384], P(('gx', 'gy'))
The draws below stay inside these ranges and needn't reach their ends.
Inputs may be any that keep to these rules, and one draw needn't show every extreme that they name: `goal_bins`: bin b belongs to owner b // 64, owners numbered in the order of gx then gy. Of the goals of one device, at most 2 fall in the bins of one owner; some owner receives exactly 2 goals from every device.
All inputs are finite; a program needn't handle non-finite values.
Results may differ from the reference program's by a relative error of at most 0.0029.
Values may be sent and summed in bfloat16 or wider, within the bound.
A program may use at most 64 MiB of HBM per device.

```python
import math
import jax
import jax.numpy as jnp

E = 128
BINS_DEV = 64
G_DEV = 128
GOALS = 32768
BINS = 16384
N_GX = 16
N_GY = 16


def draw_goal_bins(key, part):
    devices = N_GX * N_GY
    capacity = max(2, 2 * G_DEV // devices)
    key_common = jax.random.fold_in(key, 11)
    key_blocks = jax.random.fold_in(key, 12)
    key_offset = jax.random.fold_in(key, 13)
    common = jax.random.randint(key_common, (), 0, devices).astype(jnp.int32)

    def one_block(block_key):
        key_slots = jax.random.fold_in(block_key, 1)
        key_order = jax.random.fold_in(block_key, 2)
        slots = jax.random.permutation(key_slots, (devices - 1) * capacity).astype(jnp.int32)
        others = slots[:G_DEV - capacity] // capacity
        others = others + (others >= common).astype(jnp.int32)
        owners = jnp.concatenate([jnp.zeros((capacity,), jnp.int32) + common, others.astype(jnp.int32)])
        return jax.random.permutation(key_order, owners).astype(jnp.int32)
    owners = jax.vmap(one_block)(jax.random.split(key_blocks, devices)).reshape(-1)
    offsets = jax.random.randint(key_offset, (G_DEV * devices,), 0, BINS_DEV).astype(jnp.int32)
    return (owners * BINS_DEV + offsets).astype(jnp.int32)


def steps_of(rng, extent, pieces, least, high):
    gain = 1.0
    for position, shards_of in pieces:
        draws = jax.random.uniform(jax.random.fold_in(jax.random.fold_in(rng, 6), position), (shards_of,), jnp.float32, least / len(pieces), high / len(pieces))
        gain = gain * jnp.repeat(jnp.exp(draws), extent[position] // shards_of).reshape((-1,) + (1,) * (len(extent) - 1 - position))
    return gain


def gaussian(stream_key, dims, spread, reach, cuts=(), kind=jnp.bfloat16):
    array = jax.random.normal(stream_key, dims, jnp.float32) * spread
    if len(cuts) > 0:
        array = steps_of(stream_key, dims, cuts, -0.22, 0.18) * array
    return jnp.clip(array, min=-reach, max=reach).astype(kind)


def setup_inputs(seed: int = 0) -> dict:
    streams_of = jax.random.split(jax.random.key(seed), 4)
    goal_embed = gaussian(streams_of[0], (GOALS, E), 1.0, 6.0, ((0, 256),))
    goal_bins = draw_goal_bins(jax.random.fold_in(streams_of[3], 71), 0)
    goal_weights = jnp.clip(jnp.exp(math.log(10.0) - 4.6051702 * jax.random.uniform(streams_of[2], (GOALS,), jnp.float32) ** steps_of(streams_of[2], (GOALS,), ((0, 256),), -0.2, 0.2)), 0.1, 10.0)
    return {"goal_embed": goal_embed, "goal_bins": goal_bins, "goal_weights": goal_weights}


def reference(goal_embed, goal_bins, goal_weights):
    scaled = (goal_weights[:, None] * goal_embed.astype(jnp.float32)).astype(jnp.bfloat16)
    bin_sums = jax.ops.segment_sum(scaled.astype(jnp.float32), goal_bins, num_segments=BINS)
    bin_mass = jax.ops.segment_sum(goal_weights, goal_bins, num_segments=BINS)
    total_mass = jnp.sum(goal_weights)
    bin_mean = bin_sums / (bin_mass[:, None] + 1.0)
    rarity = jnp.log(total_mass / BINS) - jnp.log(bin_mass + 1.0)
    return bin_mean, rarity
```

```python
import jax
import jax.numpy as jnp
from jax import lax
from jax.experimental import pallas as pl
from jax.experimental.pallas import tpu as pltpu
from jax.sharding import Mesh
from jax.sharding import PartitionSpec as P

BINS_DEV = 64
GX_GY = ("gx_0", "gx_1", "gy_0", "gy_1", "gy_2")
LOGICAL = pl.DeviceIdType.LOGICAL
DEVICES = 256
PLANE = 32
DEPTH = 8


def depth_of(flat):
    return ((flat >> 6) << 1) | ((flat >> 3) & 1)


def place_of(flat):
    return (((flat >> 4) & 3) << 3) | (flat & 7)


def flat_of_place(place):
    return ((place >> 3) << 4) | (place & 7)


def flat_of_depth(depth):
    return ((depth >> 1) << 6) | ((depth & 1) << 3)


def remote(src, dst, send, recv, target):
    return pltpu.make_async_remote_copy(
        src_ref=src, dst_ref=dst, send_sem=send, recv_sem=recv, device_id=target, device_id_type=LOGICAL
    )


def exchange(
    embed_hbm, bins_hbm, weights_hbm, sums_ref, den_ref, log_ref,
    embed, bins, weights, packed, arrived, tags, plane_tags, column, depth_tags,
    in_sems, local_sems, send, recv, send_plane, recv_plane, send_depth, recv_depth,
):
    me = lax.axis_index(GX_GY)
    my_depth = depth_of(me)
    my_place = place_of(me)
    loads = [
        pltpu.make_async_copy(bins_hbm, bins, in_sems.at[0]),
        pltpu.make_async_copy(weights_hbm, weights, in_sems.at[1]),
        pltpu.make_async_copy(embed_hbm, embed, in_sems.at[2]),
    ]
    for load in loads:
        load.start()
    barrier = pltpu.get_barrier_semaphore()

    def greet(step, carry):
        pl.semaphore_signal(barrier, inc=1, device_id=me ^ (DEVICES - 1 - step), device_id_type=LOGICAL)
        return carry

    lax.fori_loop(0, DEVICES - 1, greet, 0, unroll=15)
    for load in loads:
        load.wait()

    lanes = lax.broadcasted_iota(jnp.int32, (128, 128), 1)
    rows = lax.broadcasted_iota(jnp.int32, (128, 128), 0)
    bin_row = jnp.broadcast_to(bins[...], (128, 128))
    weight_row = jnp.broadcast_to(weights[...], (128, 128))
    bin_col = jnp.transpose(bin_row.astype(jnp.float32)).astype(jnp.int32)
    weight_col = jnp.transpose(weight_row)
    owner_row = bin_row >> 6
    owner_col = bin_col >> 6
    earlier = jnp.where((owner_row == owner_col) & (rows < lanes), 1.0, 0.0)
    slot_of = jnp.sum(earlier, axis=0, keepdims=True).astype(jnp.int32)
    owner = bins[...] >> 6
    row_id = owner * 2 + slot_of
    tag_id = place_of(owner) * 2 + slot_of

    scaled = (weight_col * embed[...].astype(jnp.float32)).astype(jnp.bfloat16)
    pick = (lax.broadcasted_iota(jnp.int32, (2 * DEVICES, 128), 0) == row_id).astype(jnp.float32)
    packed[...] = jnp.dot(
        pick.astype(jnp.bfloat16), scaled, preferred_element_type=jnp.float32
    ).astype(jnp.bfloat16)

    lane_of = depth_of(owner_col) * 2
    offset_col = (bin_col & (BINS_DEV - 1)).astype(jnp.float32)
    values = jnp.where(lanes == lane_of, weight_col, 0.0) + jnp.where(lanes == lane_of + 1, offset_col, 0.0)
    tag_pick = (lax.broadcasted_iota(jnp.int32, (2 * PLANE, 128), 0) == tag_id).astype(jnp.float32)
    tag_lanes = lax.broadcasted_iota(jnp.int32, (2 * PLANE, 128), 1)
    tag_rows = lax.broadcasted_iota(jnp.int32, (2 * PLANE, 128), 0)
    local_total = jnp.sum(weights[...])
    tags[...] = jnp.dot(
        tag_pick, values, precision=lax.Precision.HIGHEST, preferred_element_type=jnp.float32
    ) + jnp.where((tag_lanes == 2 * DEPTH) & (tag_rows % 2 == 0), local_total, 0.0)

    pl.semaphore_wait(barrier, DEVICES - 1)

    for step in range(PLANE - 1, 0, -1):
        place = my_place ^ step
        remote(
            tags.at[pl.ds(pl.multiple_of(2 * place, 2), 2)],
            plane_tags.at[pl.ds(pl.multiple_of(2 * my_place, 2), 2)],
            send_plane, recv_plane, me ^ flat_of_place(step),
        ).start()
    my_slab = pl.ds(pl.multiple_of(2 * (my_depth * PLANE + my_place), 2), 2)

    def give(step, carry):
        target = me ^ (DEVICES - 1 - step)
        remote(
            packed.at[pl.ds(pl.multiple_of(2 * target, 2), 2)], arrived.at[my_slab], send, recv, target
        ).start()
        return carry

    lax.fori_loop(0, DEVICES - 1, give, 0, unroll=15)
    own = [
        pltpu.make_async_copy(packed.at[pl.ds(pl.multiple_of(2 * me, 2), 2)], arrived.at[my_slab], local_sems.at[0]),
        pltpu.make_async_copy(
            tags.at[pl.ds(pl.multiple_of(2 * my_place, 2), 2)],
            plane_tags.at[pl.ds(pl.multiple_of(2 * my_place, 2), 2)],
            local_sems.at[1],
        ),
    ]
    for copy in own:
        copy.start()
    for copy in own:
        copy.wait()

    others = pl.ds(0, 2 * (PLANE - 1))
    plane_all = remote(tags.at[others], plane_tags.at[others], send_plane, recv_plane, me ^ 1)
    plane_all.wait_recv()
    plane = plane_tags[...]
    plane_total = jnp.sum(jnp.where(tag_lanes == 2 * DEPTH, plane, 0.0))
    spare = jnp.where((tag_lanes < 2 * DEPTH) & (tag_lanes % 2 == 0) & (tag_rows == 0), plane_total, 0.0)
    column[...] = jnp.transpose(jnp.concatenate([plane, spare], axis=0))[: 2 * DEPTH]
    for step in range(DEPTH - 1, 0, -1):
        depth = my_depth ^ step
        remote(
            column.at[pl.ds(pl.multiple_of(2 * depth, 2), 2)],
            depth_tags.at[pl.ds(pl.multiple_of(2 * my_depth, 2), 2)],
            send_depth, recv_depth, me ^ flat_of_depth(step),
        ).start()
    mine = pl.ds(pl.multiple_of(2 * my_depth, 2), 2)
    own_column = pltpu.make_async_copy(column.at[mine], depth_tags.at[mine], local_sems.at[2])
    own_column.start()
    own_column.wait()
    others = pl.ds(0, 2 * (DEPTH - 1))
    depth_all = remote(column.at[others], depth_tags.at[others], send_depth, recv_depth, me ^ 8)
    depth_all.wait_recv()

    half = lax.broadcasted_iota(jnp.int32, (1, 128), 1) < 64
    labels = lax.broadcasted_iota(jnp.int32, (BINS_DEV, 128), 0).astype(jnp.float32)
    total = jnp.zeros((1, 1), jnp.float32)
    weighed = jnp.zeros((BINS_DEV, 128), jnp.float32)
    selectors = []
    for pair in range(DEPTH // 2):
        first = depth_tags[4 * pair : 4 * pair + 2]
        second = depth_tags[4 * pair + 2 : 4 * pair + 4]
        total = total + first[0:1, 64:65] + second[0:1, 64:65]
        turned = pltpu.roll(second, 64, axis=1)
        weight = jnp.where(half, first[0:1], turned[0:1])
        offset = jnp.where(half, first[1:2], turned[1:2])
        chosen = labels == offset
        weighed = weighed + jnp.where(chosen, weight, 0.0)
        selectors.append(jnp.where(chosen, 1.0, 0.0).astype(jnp.bfloat16))
    den = jnp.broadcast_to(jnp.sum(weighed, axis=1, keepdims=True), (BINS_DEV, 128)) + 1.0
    den_ref[...] = den
    logs = jnp.log(jnp.transpose(den)[0:1, :BINS_DEV])
    log_ref[...] = jnp.concatenate(
        [jnp.broadcast_to(jnp.log(total / (BINS_DEV * DEVICES)), (1, BINS_DEV)), logs], axis=1
    )

    most = pl.ds(0, 2 * (DEVICES - 1))
    all_data = remote(packed.at[most], arrived.at[most], send, recv, me ^ 1)
    all_data.wait_recv()
    sums_ref[...] = jnp.dot(
        jnp.concatenate(selectors, axis=1), arrived[...], preferred_element_type=jnp.float32
    )
    plane_all.wait_send()
    depth_all.wait_send()
    all_data.wait_send()


def shards(goal_embed, goal_bins, goal_weights):
    width = goal_embed.shape[1]
    goals = goal_embed.shape[0]
    vmem = pl.BlockSpec(memory_space=pltpu.VMEM)
    anywhere = pl.BlockSpec(memory_space=pl.ANY)
    dma = pltpu.SemaphoreType.DMA
    sums, den, logs = pl.pallas_call(
        exchange,
        out_shape=(
            jax.ShapeDtypeStruct((BINS_DEV, width), jnp.float32),
            jax.ShapeDtypeStruct((BINS_DEV, width), jnp.float32),
            jax.ShapeDtypeStruct((1, 2 * BINS_DEV), jnp.float32),
        ),
        in_specs=[anywhere] * 3,
        out_specs=(vmem, vmem, vmem),
        scratch_shapes=[
            pltpu.VMEM((goals, width), jnp.bfloat16),
            pltpu.VMEM((1, goals), jnp.int32),
            pltpu.VMEM((1, goals), jnp.float32),
            pltpu.VMEM((2 * DEVICES, width), jnp.bfloat16),
            pltpu.VMEM((2 * DEVICES, width), jnp.bfloat16),
            pltpu.VMEM((2 * PLANE, 128), jnp.float32),
            pltpu.VMEM((2 * PLANE, 128), jnp.float32),
            pltpu.VMEM((2 * DEPTH, 128), jnp.float32),
            pltpu.VMEM((2 * DEPTH, 128), jnp.float32),
            dma((3,)), dma((3,)),
            dma(()), dma(()), dma(()), dma(()), dma(()), dma(()),
        ],
        compiler_params=pltpu.CompilerParams(collective_id=0, has_side_effects=True),
        name="exchange",
    )(goal_embed, goal_bins.reshape(1, goals), goal_weights.reshape(1, goals))
    rarity = logs[0, :BINS_DEV] - logs[0, BINS_DEV:]
    return sums / den, rarity


def solution(mesh):
    split = Mesh(mesh.devices.reshape(4, 4, 2, 4, 2), GX_GY)
    placed = (P(GX_GY, None), P(GX_GY), P(GX_GY))
    return jax.shard_map(
        shards, mesh=split, in_specs=placed, out_specs=(P(GX_GY, None), P(GX_GY)), check_vma=False
    )
```

```python
import jax
import jax.numpy as jnp
from jax import lax
from jax.experimental import pallas as pl
from jax.experimental.pallas import tpu as pltpu
from jax.sharding import Mesh
from jax.sharding import PartitionSpec as P

BINS_DEV = 64
GX_GY = ("gx_0", "gx_1", "gy_0", "gy_1", "gy_2")
LOGICAL = pl.DeviceIdType.LOGICAL
DEVICES = 256
PLANE = 32
DEPTH = 8
HOPS = (0, 1, 2, 1)
STEPS = sorted(range(1, PLANE), key=lambda step: -(2 * HOPS[step >> 3] + 2 * HOPS[(step >> 1) & 3] + step % 2))
TURNS = (4, 3, 5, 2, 6, 1, 7)


def depth_of(flat):
    return ((flat >> 6) << 1) | ((flat >> 3) & 1)


def place_of(flat):
    return (((flat >> 4) & 3) << 3) | (flat & 7)


def flat_of_place(place):
    return ((place >> 3) << 4) | (place & 7)


def flat_of_depth(depth):
    return ((depth >> 1) << 6) | ((depth & 1) << 3)


def remote(src, dst, send, recv, target):
    return pltpu.make_async_remote_copy(
        src_ref=src, dst_ref=dst, send_sem=send, recv_sem=recv, device_id=target, device_id_type=LOGICAL
    )


def exchange(
    embed_hbm, bins_hbm, weights_hbm, sums_ref, den_ref, log_ref,
    embed, bins, weights, packed, relay, arrived, tags, plane_tags, column, depth_tags,
    in_sems, send_plane, recv_plane, send_depth, recv_depth, send_tags, recv_tags, send_column, recv_column,
):
    me = lax.axis_index(GX_GY)
    my_depth = depth_of(me)
    my_place = place_of(me)
    my_row = my_place >> 3
    bottom = flat_of_place(my_place)
    loads = [
        pltpu.make_async_copy(bins_hbm, bins, in_sems.at[0]),
        pltpu.make_async_copy(weights_hbm, weights, in_sems.at[1]),
        pltpu.make_async_copy(embed_hbm, embed, in_sems.at[2]),
    ]
    for load in loads:
        load.start()
    barrier = pltpu.get_barrier_semaphore()
    for turn in TURNS:
        depth = (my_depth + turn) & (DEPTH - 1)
        pl.semaphore_signal(barrier, inc=1, device_id=bottom | flat_of_depth(depth), device_id_type=LOGICAL)
    for step in STEPS:
        pl.semaphore_signal(barrier, inc=1, device_id=me ^ flat_of_place(step), device_id_type=LOGICAL)
    for load in loads:
        load.wait()

    lanes = lax.broadcasted_iota(jnp.int32, (128, 128), 1)
    rows = lax.broadcasted_iota(jnp.int32, (128, 128), 0)
    bin_row = jnp.broadcast_to(bins[...], (128, 128))
    weight_row = jnp.broadcast_to(weights[...], (128, 128))
    bin_col = jnp.transpose(bin_row.astype(jnp.float32)).astype(jnp.int32)
    weight_col = jnp.transpose(weight_row)
    owner_row = bin_row >> 6
    owner_col = bin_col >> 6
    earlier = jnp.where((owner_row == owner_col) & (rows < lanes), 1.0, 0.0)
    slot_of = jnp.sum(earlier, axis=0, keepdims=True).astype(jnp.int32)
    owner = bins[...] >> 6
    row_id = (place_of(owner) * DEPTH + depth_of(owner)) * 2 + slot_of
    tag_id = place_of(owner) * 2 + slot_of

    lane_of = depth_of(owner_col) * 2
    offset_col = (bin_col & (BINS_DEV - 1)).astype(jnp.float32)
    values = jnp.where(lanes == lane_of, weight_col, 0.0) + jnp.where(lanes == lane_of + 1, offset_col, 0.0)
    tag_pick = (lax.broadcasted_iota(jnp.int32, (2 * PLANE, 128), 0) == tag_id).astype(jnp.float32)
    tag_lanes = lax.broadcasted_iota(jnp.int32, (2 * PLANE, 128), 1)
    tag_rows = lax.broadcasted_iota(jnp.int32, (2 * PLANE, 128), 0)
    local_total = jnp.sum(weights[...])
    tags[...] = jnp.dot(
        tag_pick, values, precision=lax.Precision.HIGHEST, preferred_element_type=jnp.float32
    ) + jnp.where((tag_lanes == 2 * DEPTH) & (tag_rows % 2 == 0), local_total, 0.0)

    scaled = (weight_col * embed[...].astype(jnp.float32)).astype(jnp.bfloat16)
    pick = (lax.broadcasted_iota(jnp.int32, (2 * DEVICES, 128), 0) == row_id).astype(jnp.float32)
    packed.reshape(2 * DEVICES, 128)[...] = jnp.dot(
        pick.astype(jnp.bfloat16), scaled, preferred_element_type=jnp.float32
    ).astype(jnp.bfloat16)

    pl.semaphore_wait(barrier, PLANE - 1 + DEPTH - 1)

    my_tags = pl.ds(pl.multiple_of(2 * my_place, 2), 2)
    for step in STEPS:
        place = my_place ^ step
        remote(
            tags.at[pl.ds(pl.multiple_of(2 * place, 2), 2)], plane_tags.at[my_tags],
            send_tags, recv_tags, me ^ flat_of_place(step),
        ).start()
    for step in STEPS:
        remote(
            packed.at[my_place ^ step], relay.at[my_place],
            send_plane, recv_plane.at[step >> 3], me ^ flat_of_place(step),
        ).start()
    relay[my_place] = packed[my_place]
    plane_tags[my_tags] = tags[my_tags]

    def pass_on(group):
        count = 8 if group else 7
        remote(
            packed.at[pl.ds(0, count)], relay.at[pl.ds(0, count)], send_plane, recv_plane.at[group], me ^ 1
        ).wait_recv()
        members = pl.ds(pl.multiple_of((my_row ^ group) * 8, 8), 8)
        for turn in TURNS:
            depth = (my_depth + turn) & (DEPTH - 1)
            remote(
                relay.at[members, depth], arrived.at[my_depth, members],
                send_depth, recv_depth, bottom | flat_of_depth(depth),
            ).start()
        arrived[my_depth, members] = relay[members, my_depth]

    for group in (0, 1, 3):
        pass_on(group)

    others = pl.ds(0, 2 * (PLANE - 1))
    plane_all = remote(tags.at[others], plane_tags.at[others], send_tags, recv_tags, me ^ 1)
    plane_all.wait_recv()
    plane = plane_tags[...]
    plane_total = jnp.sum(jnp.where(tag_lanes == 2 * DEPTH, plane, 0.0))
    spare = jnp.where((tag_lanes < 2 * DEPTH) & (tag_lanes % 2 == 0) & (tag_rows == 0), plane_total, 0.0)
    column[...] = jnp.transpose(jnp.concatenate([plane, spare], axis=0))[: 2 * DEPTH]
    mine = pl.ds(pl.multiple_of(2 * my_depth, 2), 2)
    for turn in TURNS:
        depth = (my_depth + turn) & (DEPTH - 1)
        remote(
            column.at[pl.ds(pl.multiple_of(2 * depth, 2), 2)], depth_tags.at[mine],
            send_column, recv_column, bottom | flat_of_depth(depth),
        ).start()
    depth_tags[mine] = column[mine]
    pass_on(2)

    others = pl.ds(0, 2 * (DEPTH - 1))
    depth_all = remote(column.at[others], depth_tags.at[others], send_column, recv_column, me ^ 8)
    depth_all.wait_recv()

    half = lax.broadcasted_iota(jnp.int32, (1, 128), 1) < 64
    labels = lax.broadcasted_iota(jnp.int32, (BINS_DEV, 128), 0).astype(jnp.float32)
    total = jnp.zeros((1, 1), jnp.float32)
    weighed = jnp.zeros((BINS_DEV, 128), jnp.float32)
    selectors = []
    for pair in range(DEPTH // 2):
        first = depth_tags[4 * pair : 4 * pair + 2]
        second = depth_tags[4 * pair + 2 : 4 * pair + 4]
        total = total + first[0:1, 64:65] + second[0:1, 64:65]
        turned = pltpu.roll(second, 64, axis=1)
        weight = jnp.where(half, first[0:1], turned[0:1])
        offset = jnp.where(half, first[1:2], turned[1:2])
        chosen = labels == offset
        weighed = weighed + jnp.where(chosen, weight, 0.0)
        selectors.append(jnp.where(chosen, 1.0, 0.0).astype(jnp.bfloat16))
    den = jnp.broadcast_to(jnp.sum(weighed, axis=1, keepdims=True), (BINS_DEV, 128)) + 1.0
    den_ref[...] = den
    logs = jnp.log(jnp.transpose(den)[0:1, :BINS_DEV])
    log_ref[...] = jnp.concatenate(
        [jnp.broadcast_to(jnp.log(total / (BINS_DEV * DEVICES)), (1, BINS_DEV)), logs], axis=1
    )

    depth_most = arrived.at[pl.ds(0, DEPTH - 1)]
    depth_data = remote(depth_most, depth_most, send_depth, recv_depth, me ^ 8)
    depth_data.wait_recv()
    sums_ref[...] = jnp.dot(
        jnp.concatenate(selectors, axis=1), arrived.reshape(2 * DEVICES, 128)[...],
        preferred_element_type=jnp.float32,
    )
    most = pl.ds(0, PLANE - 1)
    remote(packed.at[most], relay.at[most], send_plane, recv_plane.at[0], me ^ 1).wait_send()
    plane_all.wait_send()
    depth_all.wait_send()
    depth_data.wait_send()


def shards(goal_embed, goal_bins, goal_weights):
    width = goal_embed.shape[1]
    goals = goal_embed.shape[0]
    vmem = pl.BlockSpec(memory_space=pltpu.VMEM)
    anywhere = pl.BlockSpec(memory_space=pltpu.HBM)
    dma = pltpu.SemaphoreType.DMA
    sums, den, logs = pl.pallas_call(
        exchange,
        out_shape=(
            jax.ShapeDtypeStruct((BINS_DEV, width), jnp.float32),
            jax.ShapeDtypeStruct((BINS_DEV, width), jnp.float32),
            jax.ShapeDtypeStruct((1, 2 * BINS_DEV), jnp.float32),
        ),
        in_specs=[anywhere] * 3,
        out_specs=(vmem, vmem, vmem),
        scratch_shapes=[
            pltpu.VMEM((goals, width), jnp.bfloat16),
            pltpu.VMEM((1, goals), jnp.int32),
            pltpu.VMEM((1, goals), jnp.float32),
            pltpu.VMEM((PLANE, DEPTH, 2, width), jnp.bfloat16),
            pltpu.VMEM((PLANE, DEPTH, 2, width), jnp.bfloat16),
            pltpu.VMEM((DEPTH, PLANE, 2, width), jnp.bfloat16),
            pltpu.VMEM((2 * PLANE, 128), jnp.float32),
            pltpu.VMEM((2 * PLANE, 128), jnp.float32),
            pltpu.VMEM((2 * DEPTH, 128), jnp.float32),
            pltpu.VMEM((2 * DEPTH, 128), jnp.float32),
            dma((3,)), dma(()), dma((4,)), dma(()), dma(()), dma(()), dma(()), dma(()), dma(()),
        ],
        compiler_params=pltpu.CompilerParams(collective_id=0, has_side_effects=True, vmem_limit_bytes=4 << 20),
        name="exchange",
    )(*[
        pltpu.with_memory_space_constraint(array, pltpu.HBM)
        for array in (goal_embed, goal_bins.reshape(1, goals), goal_weights.reshape(1, goals))
    ])
    rarity = logs[0, :BINS_DEV] - logs[0, BINS_DEV:]
    return sums / den, rarity


def solution(mesh):
    split = Mesh(mesh.devices.reshape(4, 4, 2, 4, 2), GX_GY)
    placed = (P(GX_GY, None), P(GX_GY), P(GX_GY))
    return jax.shard_map(
        shards, mesh=split, in_specs=placed, out_specs=(P(GX_GY, None), P(GX_GY)), check_vma=False
    )
```

```python
import jax
import jax.numpy as jnp
from jax import lax
from jax.experimental import pallas as pl
from jax.experimental.pallas import tpu as pltpu
from jax.sharding import Mesh
from jax.sharding import PartitionSpec as P

BINS_DEV = 64
AXIS = "device"
LOGICAL = pl.DeviceIdType.LOGICAL
DEVICES = 256
CHIPS = 16
PLANE = 32
DEPTH = 8
HOPS = (0, 1, 2, 1)
STEPS = sorted(range(1, CHIPS), key=lambda step: -(HOPS[step >> 2] + HOPS[step & 3]))
GROUPS = (0, 3, 1, 2)


def depth_of(flat):
    return ((flat >> 6) << 1) | ((flat >> 3) & 1)


def chip_of(flat):
    return (((flat >> 4) & 3) << 2) | ((flat >> 1) & 3)


def flat_of_chip(chip):
    return ((chip >> 2) << 4) | ((chip & 3) << 1)


def flat_of_depth(depth):
    return ((depth >> 1) << 6) | ((depth & 1) << 3)


def remote(src, dst, send, recv, target):
    return pltpu.make_async_remote_copy(
        src_ref=src, dst_ref=dst, send_sem=send, recv_sem=recv, device_id=target, device_id_type=LOGICAL
    )


def two(index):
    return pl.ds(pl.multiple_of(2 * index, 2), 2)


def exchange(
    embed_hbm, bins_hbm, weights_hbm, mean_ref, rarity_ref,
    embed, bins, weights, packed, relay, arrived, tags, plane_tags, column, depth_tags,
    in_sems, send_plane, recv_plane, send_depth, recv_depth,
    send_tags, recv_tags, send_column, recv_column, column_ready,
):
    me = lax.axis_index(AXIS)
    core = me & 1
    my_depth = depth_of(me)
    my_chip = chip_of(me)
    my_place = my_chip * 2 + core
    my_row = my_chip >> 2
    bottom = flat_of_chip(my_chip)
    loads = [
        pltpu.make_async_copy(bins_hbm, bins, in_sems.at[0]),
        pltpu.make_async_copy(weights_hbm, weights, in_sems.at[1]),
        pltpu.make_async_copy(embed_hbm, embed, in_sems.at[2]),
    ]
    for load in loads:
        load.start()
    barrier = pltpu.get_barrier_semaphore()

    def greet(target):
        pl.semaphore_signal(barrier, inc=1, device_id=target, device_id_type=LOGICAL)

    def column_core(turn):
        depth = turn + (turn >= my_depth).astype(jnp.int32)
        return depth, bottom | flat_of_depth(depth) | 1

    greet(me ^ 1)

    @pl.when(core == 1)
    def _():
        for step in STEPS:
            greet(me ^ flat_of_chip(step))
            greet(me ^ flat_of_chip(step) ^ 1)
        for turn in range(DEPTH - 1):
            greet(column_core(turn)[1])

    for load in loads:
        load.wait()

    lanes = lax.broadcasted_iota(jnp.int32, (128, 128), 1)
    rows = lax.broadcasted_iota(jnp.int32, (128, 128), 0)
    bin_row = jnp.broadcast_to(bins[...], (128, 128))
    weight_row = jnp.broadcast_to(weights[...], (128, 128))
    bin_col = jnp.transpose(bin_row.astype(jnp.float32)).astype(jnp.int32)
    weight_col = jnp.transpose(weight_row)
    owner_row = bin_row >> 6
    owner_col = bin_col >> 6
    earlier = jnp.where((owner_row == owner_col) & (rows < lanes), 1.0, 0.0)
    slot_of = jnp.sum(earlier, axis=0, keepdims=True).astype(jnp.int32)
    owner = bins[...] >> 6
    row_id = ((chip_of(owner) * DEPTH + depth_of(owner)) * 2 + (owner & 1)) * 2 + slot_of
    tag_id = chip_of(owner) * 2 + slot_of

    lane_of = (depth_of(owner_col) * 2 + (owner_col & 1)) * 2
    offset_col = (bin_col & (BINS_DEV - 1)).astype(jnp.float32)
    values = jnp.where(lanes == lane_of, weight_col, 0.0) + jnp.where(lanes == lane_of + 1, offset_col, 0.0)
    tag_lanes = lax.broadcasted_iota(jnp.int32, (2 * CHIPS, 128), 1)
    tag_rows = lax.broadcasted_iota(jnp.int32, (2 * CHIPS, 128), 0)
    tag_pick = (tag_rows == tag_id).astype(jnp.float32)
    local_total = jnp.sum(weights[...])
    tags[...] = jnp.dot(
        tag_pick, values, precision=lax.Precision.HIGHEST, preferred_element_type=jnp.float32
    ) + jnp.where((tag_lanes == 4 * DEPTH) & (tag_rows % 2 == 0), local_total, 0.0)

    scaled = (weight_col * embed[...].astype(jnp.float32)).astype(jnp.bfloat16)
    pick = (lax.broadcasted_iota(jnp.int32, (2 * DEVICES, 128), 0) == row_id).astype(jnp.float32)
    packed.reshape(2 * DEVICES, 128)[...] = jnp.dot(
        pick.astype(jnp.bfloat16), scaled, preferred_element_type=jnp.float32
    ).astype(jnp.bfloat16)

    def hand_tags(chip, target):
        remote(tags.at[two(chip)], plane_tags.at[two(my_place)], send_tags, recv_tags, target).start()

    def hand_data(chip, target, group):
        remote(packed.at[chip], relay.at[my_place], send_plane, recv_plane.at[group], target).start()

    def hand_all():
        for step in STEPS:
            hand_tags(my_chip ^ step, (me ^ flat_of_chip(step)) | 1)
        for step in STEPS:
            hand_data(my_chip ^ step, (me ^ flat_of_chip(step)) | 1, step >> 2)

    everything = arrived.at[pl.ds(0, DEPTH)]
    all_tags = pl.ds(0, 2 * DEPTH)

    @pl.when(core == 0)
    def _():
        pl.semaphore_wait(barrier, CHIPS)
        hand_all()
        hand_tags(my_chip, me ^ 1)
        hand_data(my_chip, me ^ 1, 0)
        remote(depth_tags.at[all_tags], depth_tags.at[all_tags], send_column, recv_column, me ^ 1).wait_recv()

    @pl.when(core == 1)
    def _():
        pl.semaphore_wait(barrier, CHIPS - 1 + DEPTH - 1 + 1)
        hand_all()
        for turn in range(DEPTH - 1):
            pl.semaphore_signal(column_ready, inc=1, device_id=column_core(turn)[1], device_id_type=LOGICAL)
        relay[my_place] = packed[my_chip]
        plane_tags[two(my_place)] = tags[two(my_chip)]
        pl.semaphore_wait(column_ready, DEPTH - 1)

        def pass_on(group):
            count = 8 if group else 7
            part = relay.at[pl.ds(0, count)]
            remote(part, part, send_plane, recv_plane.at[group], me ^ 1).wait_recv()
            members = pl.ds(pl.multiple_of((my_row ^ group) * 8, 8), 8)
            for turn in range(DEPTH - 1):
                depth, target = column_core(turn)
                for side in (0, 1):
                    remote(
                        relay.at[members, depth * 2 + side], arrived.at[my_depth, members],
                        send_depth, recv_depth, target ^ 1 ^ side,
                    ).start()
            remote(
                relay.at[members, my_depth * 2], arrived.at[my_depth, members], send_depth, recv_depth, me ^ 1
            ).start()
            arrived[my_depth, members] = relay[members, my_depth * 2 + 1]

        for group in GROUPS[:3]:
            pass_on(group)

        others = plane_tags.at[pl.ds(0, 2 * (PLANE - 1))]
        remote(others, others, send_tags, recv_tags, me ^ 1).wait_recv()
        plane = plane_tags[...]
        wide_lanes = lax.broadcasted_iota(jnp.int32, (2 * PLANE, 128), 1)
        wide_rows = lax.broadcasted_iota(jnp.int32, (2 * PLANE, 128), 0)
        plane_total = jnp.sum(jnp.where(wide_lanes == 4 * DEPTH, plane, 0.0))
        spare = jnp.where(
            (wide_lanes < 4 * DEPTH) & (wide_lanes % 2 == 0) & (wide_rows == 0), plane_total, 0.0
        )
        column[...] = jnp.transpose(jnp.concatenate([plane, spare], axis=0))[: 4 * DEPTH]
        for turn in range(DEPTH - 1):
            depth, target = column_core(turn)
            for side in (0, 1):
                remote(
                    column.at[two(depth * 2 + side)], depth_tags.at[two(my_depth)],
                    send_column, recv_column, target ^ 1 ^ side,
                ).start()
        remote(
            column.at[two(my_depth * 2)], depth_tags.at[two(my_depth)], send_column, recv_column, me ^ 1
        ).start()
        depth_tags[two(my_depth)] = column[two(my_depth * 2 + 1)]
        pass_on(GROUPS[3])
        most = depth_tags.at[pl.ds(0, 2 * (DEPTH - 1))]
        remote(most, most, send_column, recv_column, me ^ 1).wait_recv()

    half = lax.broadcasted_iota(jnp.int32, (1, 128), 1) < 64
    labels = lax.broadcasted_iota(jnp.int32, (BINS_DEV, 128), 0).astype(jnp.float32)
    total = jnp.zeros((1, 1), jnp.float32)
    weighed = jnp.zeros((BINS_DEV, 128), jnp.float32)
    selectors = []
    for pair in range(DEPTH // 2):
        first = depth_tags[4 * pair : 4 * pair + 2]
        second = depth_tags[4 * pair + 2 : 4 * pair + 4]
        total = total + first[0:1, 64:65] + second[0:1, 64:65]
        turned = pltpu.roll(second, 64, axis=1)
        weight = jnp.where(half, first[0:1], turned[0:1])
        offset = jnp.where(half, first[1:2], turned[1:2])
        chosen = labels == offset
        weighed = weighed + jnp.where(chosen, weight, 0.0)
        selectors.append(jnp.where(chosen, 1.0, 0.0).astype(jnp.bfloat16))
    den = jnp.broadcast_to(jnp.sum(weighed, axis=1, keepdims=True), (BINS_DEV, 128)) + 1.0
    rarity_ref[...] = jnp.log(total / (BINS_DEV * DEVICES)) - jnp.log(jnp.transpose(den)[0:1, :BINS_DEV])

    @pl.when(core == 0)
    def _():
        remote(everything, everything, send_depth, recv_depth, me ^ 1).wait_recv()

    @pl.when(core == 1)
    def _():
        most = arrived.at[pl.ds(0, DEPTH - 1)]
        remote(most, most, send_depth, recv_depth, me ^ 1).wait_recv()

    mean_ref[...] = jnp.dot(
        jnp.concatenate(selectors, axis=1), arrived.reshape(2 * DEVICES, 128)[...],
        preferred_element_type=jnp.float32,
    ) / den

    def sent(chips):
        part = packed.at[pl.ds(0, chips)]
        remote(part, part, send_plane, recv_plane.at[0], me ^ 1).wait_send()
        part = tags.at[pl.ds(0, 2 * chips)]
        remote(part, part, send_tags, recv_tags, me ^ 1).wait_send()

    @pl.when(core == 0)
    def _():
        sent(CHIPS)

    @pl.when(core == 1)
    def _():
        sent(CHIPS - 1)
        part = relay.at[pl.ds(0, 2 * (2 * DEPTH - 1))]
        remote(part, part, send_depth, recv_depth, me ^ 1).wait_send()
        part = column.at[pl.ds(0, 2 * (2 * DEPTH - 1))]
        remote(part, part, send_column, recv_column, me ^ 1).wait_send()


def write_out(mean, rarity, mean_hbm, rarity_hbm, sems):
    copies = [
        pltpu.make_async_copy(mean, mean_hbm, sems.at[0]),
        pltpu.make_async_copy(rarity, rarity_hbm, sems.at[1]),
    ]
    for copy in copies:
        copy.start()
    for copy in copies:
        copy.wait()


def shards(goal_embed, goal_bins, goal_weights):
    width = goal_embed.shape[1]
    goals = goal_embed.shape[0]
    vmem = pl.BlockSpec(memory_space=pltpu.VMEM)
    hbm = pl.BlockSpec(memory_space=pltpu.HBM)
    dma = pltpu.SemaphoreType.DMA
    shapes = (
        jax.ShapeDtypeStruct((BINS_DEV, width), jnp.float32),
        jax.ShapeDtypeStruct((1, BINS_DEV), jnp.float32),
    )
    results = pl.pallas_call(
        exchange,
        out_shape=shapes,
        in_specs=[hbm] * 3,
        out_specs=(vmem, vmem),
        scratch_shapes=[
            pltpu.VMEM((goals, width), jnp.bfloat16),
            pltpu.VMEM((1, goals), jnp.int32),
            pltpu.VMEM((1, goals), jnp.float32),
            pltpu.VMEM((CHIPS, 2 * DEPTH, 2, width), jnp.bfloat16),
            pltpu.VMEM((PLANE, 2 * DEPTH, 2, width), jnp.bfloat16),
            pltpu.VMEM((DEPTH, PLANE, 2, width), jnp.bfloat16),
            pltpu.VMEM((2 * CHIPS, 128), jnp.float32),
            pltpu.VMEM((2 * PLANE, 128), jnp.float32),
            pltpu.VMEM((4 * DEPTH, 128), jnp.float32),
            pltpu.VMEM((2 * DEPTH, 128), jnp.float32),
            dma((3,)), dma(()), dma((4,)), dma(()), dma(()), dma(()), dma(()), dma(()), dma(()),
            pltpu.SemaphoreType.REGULAR,
        ],
        compiler_params=pltpu.CompilerParams(collective_id=0, has_side_effects=True, vmem_limit_bytes=4 << 20),
        name="exchange",
    )(*[
        pltpu.with_memory_space_constraint(array, pltpu.HBM)
        for array in (goal_embed, goal_bins.reshape(1, goals), goal_weights.reshape(1, goals))
    ])
    mean, rarity = pl.pallas_call(
        write_out,
        out_shape=shapes,
        in_specs=[vmem, vmem],
        out_specs=(hbm, hbm),
        scratch_shapes=[dma((2,))],
        compiler_params=pltpu.CompilerParams(vmem_limit_bytes=1 << 20),
        name="write_out",
    )(*results)
    return mean, rarity[0]


def solution(mesh):
    flat = Mesh(mesh.devices.reshape(-1), (AXIS,))
    return jax.shard_map(
        shards, mesh=flat, in_specs=(P(AXIS, None), P(AXIS), P(AXIS)),
        out_specs=(P(AXIS, None), P(AXIS)), check_vma=False,
    )
```

```python
import functools

import jax
import jax.numpy as jnp
from jax import lax
from jax.experimental import pallas as pl
from jax.experimental.pallas import tpu as pltpu
from jax.sharding import Mesh
from jax.sharding import PartitionSpec as P

BINS_DEV = 64
AXIS = "device"
LOGICAL = pl.DeviceIdType.LOGICAL
DEVICES = 256
CHIPS = 16
PLANE = 32
DEPTH = 8
HOPS = (0, 1, 2, 1)
STEPS = sorted(range(1, CHIPS), key=lambda step: -(HOPS[step >> 2] + HOPS[step & 3]))
GROUPS = (0, 3, 1, 2)
FIRST = 1
FIRST_LOTS = pl.ds(0, 2 * FIRST)
REST_LOTS = pl.ds(2 * FIRST, 2 * (DEPTH - FIRST))


def depth_of(flat):
    return ((flat >> 6) << 1) | ((flat >> 3) & 1)


def chip_of(flat):
    return (((flat >> 4) & 3) << 2) | ((flat >> 1) & 3)


def flat_of_chip(chip):
    return ((chip >> 2) << 4) | ((chip & 3) << 1)


def flat_of_depth(depth):
    return ((depth >> 1) << 6) | ((depth & 1) << 3)


def remote(src, dst, send, recv, target):
    return pltpu.make_async_remote_copy(
        src_ref=src, dst_ref=dst, send_sem=send, recv_sem=recv, device_id=target, device_id_type=LOGICAL
    )


def two(index):
    return pl.ds(pl.multiple_of(2 * index, 2), 2)


def exchange(
    embed_hbm, bins_hbm, weights_hbm, mean_ref, rarity_ref,
    embed, bins, weights, packed, relay, arrived, tags, plane_tags, column, depth_tags,
    in_sems, send_plane, recv_plane, recv_rest, send_depth, recv_depth,
    send_tags, recv_tags, send_column, recv_column, column_ready,
):
    me = lax.axis_index(AXIS)
    core = me & 1
    my_depth = depth_of(me)
    my_chip = chip_of(me)
    my_place = my_chip * 2 + core
    my_row = my_chip >> 2
    bottom = flat_of_chip(my_chip)
    loads = [
        pltpu.make_async_copy(bins_hbm, bins, in_sems.at[0]),
        pltpu.make_async_copy(weights_hbm, weights, in_sems.at[1]),
        pltpu.make_async_copy(embed_hbm, embed, in_sems.at[2]),
    ]
    for load in loads:
        load.start()
    barrier = pltpu.get_barrier_semaphore()

    def greet(target):
        pl.semaphore_signal(barrier, inc=1, device_id=target, device_id_type=LOGICAL)

    def other_relay(turn):
        return bottom | flat_of_depth(turn + (turn >= my_depth).astype(jnp.int32)) | 1

    greet(me ^ 1)

    @pl.when(core == 1)
    def _():
        for step in STEPS:
            greet(me ^ flat_of_chip(step))
            greet(me ^ flat_of_chip(step) ^ 1)
        for turn in range(DEPTH - 1):
            greet(other_relay(turn))

    for load in loads:
        load.wait()

    lanes = lax.broadcasted_iota(jnp.int32, (128, 128), 1)
    rows = lax.broadcasted_iota(jnp.int32, (128, 128), 0)
    bin_row = jnp.broadcast_to(bins[...], (128, 128))
    weight_row = jnp.broadcast_to(weights[...], (128, 128))
    bin_col = jnp.transpose(bin_row.astype(jnp.float32)).astype(jnp.int32)
    weight_col = jnp.transpose(weight_row)
    owner_row = bin_row >> 6
    owner_col = bin_col >> 6
    earlier = jnp.where((owner_row == owner_col) & (rows < lanes), 1.0, 0.0)
    slot_of = jnp.sum(earlier, axis=0, keepdims=True).astype(jnp.int32)
    owner = bins[...] >> 6
    row_id = ((chip_of(owner) * DEPTH + depth_of(owner)) * 2 + (owner & 1)) * 2 + slot_of
    tag_id = chip_of(owner) * 2 + slot_of

    lane_of = (depth_of(owner_col) * 2 + (owner_col & 1)) * 2
    offset_col = (bin_col & (BINS_DEV - 1)).astype(jnp.float32)
    values = jnp.where(lanes == lane_of, weight_col, 0.0) + jnp.where(lanes == lane_of + 1, offset_col, 0.0)
    tag_lanes = lax.broadcasted_iota(jnp.int32, (2 * CHIPS, 128), 1)
    tag_rows = lax.broadcasted_iota(jnp.int32, (2 * CHIPS, 128), 0)
    tag_pick = (tag_rows == tag_id).astype(jnp.float32)
    local_total = jnp.sum(weights[...])
    tags[...] = jnp.dot(
        tag_pick, values, precision=lax.Precision.HIGHEST, preferred_element_type=jnp.float32
    ) + jnp.where((tag_lanes == 4 * DEPTH) & (tag_rows % 2 == 0), local_total, 0.0)

    scaled = (weight_col * embed[...].astype(jnp.float32)).astype(jnp.bfloat16)
    pick = (lax.broadcasted_iota(jnp.int32, (2 * DEVICES, 128), 0) == row_id).astype(jnp.float32)
    packed.reshape(2 * DEVICES, 128)[...] = jnp.dot(
        pick.astype(jnp.bfloat16), scaled, preferred_element_type=jnp.float32
    ).astype(jnp.bfloat16)

    def hand_tags(chip, target):
        remote(tags.at[two(chip)], plane_tags.at[two(my_place)], send_tags, recv_tags, target).start()

    def hand_first(chip, target, group):
        remote(
            packed.at[chip, FIRST_LOTS], relay.at[my_place, FIRST_LOTS],
            send_plane, recv_plane.at[group], target,
        ).start()

    def hand_rest(chip, target):
        remote(
            packed.at[chip, REST_LOTS], relay.at[my_place, REST_LOTS], send_plane, recv_rest, target
        ).start()

    def hand_all():
        for step in STEPS:
            hand_tags(my_chip ^ step, (me ^ flat_of_chip(step)) | 1)
            hand_first(my_chip ^ step, (me ^ flat_of_chip(step)) | 1, step >> 2)

    everything = arrived.at[pl.ds(0, DEPTH)]
    all_tags = pl.ds(0, 2 * DEPTH)

    @pl.when(core == 0)
    def _():
        pl.semaphore_wait(barrier, CHIPS)
        hand_all()
        hand_tags(my_chip, me ^ 1)
        hand_first(my_chip, me ^ 1, 0)
        for step in STEPS:
            hand_rest(my_chip ^ step, (me ^ flat_of_chip(step)) | 1)
        hand_rest(my_chip, me ^ 1)
        remote(depth_tags.at[all_tags], depth_tags.at[all_tags], send_column, recv_column, me ^ 1).wait_recv()

    @pl.when(core == 1)
    def _():
        pl.semaphore_wait(barrier, CHIPS - 1 + DEPTH - 1 + 1)
        hand_all()
        for step in STEPS:
            hand_rest(my_chip ^ step, (me ^ flat_of_chip(step)) | 1)
        for turn in range(DEPTH - 1):
            pl.semaphore_signal(column_ready, inc=1, device_id=other_relay(turn), device_id_type=LOGICAL)
        relay[my_place] = packed[my_chip]
        plane_tags[two(my_place)] = tags[two(my_chip)]
        pl.semaphore_wait(column_ready, DEPTH - 1)

        def both_cores(depths, send_to):
            for depth in depths:
                column_at = bottom | flat_of_depth(depth)
                send_to(column_at, 2 * depth)
                pl.when(my_depth != depth)(functools.partial(send_to, column_at | 1, 2 * depth + 1))

        def pass_on(group):
            count = 8 if group else 7
            part = relay.at[pl.ds(0, count), FIRST_LOTS]
            remote(part, part, send_plane, recv_plane.at[group], me ^ 1).wait_recv()
            members = pl.ds(pl.multiple_of((my_row ^ group) * 8, 8), 8)

            def send_to(target, lot):
                remote(
                    relay.at[members, lot], arrived.at[my_depth, members], send_depth, recv_depth, target
                ).start()

            both_cores(range(FIRST), send_to)

        for group in GROUPS[:3]:
            pass_on(group)

        others = plane_tags.at[pl.ds(0, 2 * (PLANE - 1))]
        remote(others, others, send_tags, recv_tags, me ^ 1).wait_recv()
        plane = plane_tags[...]
        wide_lanes = lax.broadcasted_iota(jnp.int32, (2 * PLANE, 128), 1)
        wide_rows = lax.broadcasted_iota(jnp.int32, (2 * PLANE, 128), 0)
        plane_total = jnp.sum(jnp.where(wide_lanes == 4 * DEPTH, plane, 0.0))
        spare = jnp.where(
            (wide_lanes < 4 * DEPTH) & (wide_lanes % 2 == 0) & (wide_rows == 0), plane_total, 0.0
        )
        column[...] = jnp.transpose(jnp.concatenate([plane, spare], axis=0))[: 4 * DEPTH]

        def send_column_to(target, lot):
            remote(
                column.at[two(lot)], depth_tags.at[two(my_depth)], send_column, recv_column, target
            ).start()

        both_cores(range(DEPTH), send_column_to)
        depth_tags[two(my_depth)] = column[two(my_depth * 2 + 1)]
        pass_on(GROUPS[3])
        part = relay.at[pl.ds(0, PLANE - 1), REST_LOTS]
        remote(part, part, send_plane, recv_rest, me ^ 1).wait_recv()

        def send_rest_to(target, lot):
            remote(relay.at[:, lot], arrived.at[my_depth], send_depth, recv_depth, target).start()

        both_cores(range(FIRST, DEPTH), send_rest_to)
        arrived[my_depth] = relay[:, my_depth * 2 + 1]
        most = depth_tags.at[pl.ds(0, 2 * (DEPTH - 1))]
        remote(most, most, send_column, recv_column, me ^ 1).wait_recv()

    half = lax.broadcasted_iota(jnp.int32, (1, 128), 1) < 64
    labels = lax.broadcasted_iota(jnp.int32, (BINS_DEV, 128), 0).astype(jnp.float32)
    total = jnp.zeros((1, 1), jnp.float32)
    weighed = jnp.zeros((BINS_DEV, 128), jnp.float32)
    selectors = []
    for pair in range(DEPTH // 2):
        first = depth_tags[4 * pair : 4 * pair + 2]
        second = depth_tags[4 * pair + 2 : 4 * pair + 4]
        total = total + first[0:1, 64:65] + second[0:1, 64:65]
        turned = pltpu.roll(second, 64, axis=1)
        weight = jnp.where(half, first[0:1], turned[0:1])
        offset = jnp.where(half, first[1:2], turned[1:2])
        chosen = labels == offset
        weighed = weighed + jnp.where(chosen, weight, 0.0)
        selectors.append(jnp.where(chosen, 1.0, 0.0).astype(jnp.bfloat16))
    den = jnp.broadcast_to(jnp.sum(weighed, axis=1, keepdims=True), (BINS_DEV, 128)) + 1.0
    rarity_ref[...] = jnp.log(total / (BINS_DEV * DEVICES)) - jnp.log(jnp.transpose(den)[0:1, :BINS_DEV])

    @pl.when(core == 0)
    def _():
        remote(everything, everything, send_depth, recv_depth, me ^ 1).wait_recv()

    @pl.when(core == 1)
    def _():
        most = arrived.at[pl.ds(0, DEPTH - 1)]
        remote(most, most, send_depth, recv_depth, me ^ 1).wait_recv()

    mean_ref[...] = jnp.dot(
        jnp.concatenate(selectors, axis=1), arrived.reshape(2 * DEVICES, 128)[...],
        preferred_element_type=jnp.float32,
    ) / den

    def sent(chips):
        part = packed.at[pl.ds(0, chips)]
        remote(part, part, send_plane, recv_plane.at[0], me ^ 1).wait_send()
        part = tags.at[pl.ds(0, 2 * chips)]
        remote(part, part, send_tags, recv_tags, me ^ 1).wait_send()

    @pl.when(core == 0)
    def _():
        sent(CHIPS)

    @pl.when(core == 1)
    def _():
        sent(CHIPS - 1)
        part = relay.at[pl.ds(0, 2 * (2 * DEPTH - 1))]
        remote(part, part, send_depth, recv_depth, me ^ 1).wait_send()
        part = column.at[pl.ds(0, 2 * (2 * DEPTH - 1))]
        remote(part, part, send_column, recv_column, me ^ 1).wait_send()


def write_out(mean, rarity, mean_hbm, rarity_hbm, sems):
    copies = [
        pltpu.make_async_copy(mean, mean_hbm, sems.at[0]),
        pltpu.make_async_copy(rarity, rarity_hbm, sems.at[1]),
    ]
    for copy in copies:
        copy.start()
    for copy in copies:
        copy.wait()


def shards(goal_embed, goal_bins, goal_weights):
    width = goal_embed.shape[1]
    goals = goal_embed.shape[0]
    vmem = pl.BlockSpec(memory_space=pltpu.VMEM)
    hbm = pl.BlockSpec(memory_space=pltpu.HBM)
    dma = pltpu.SemaphoreType.DMA
    shapes = (
        jax.ShapeDtypeStruct((BINS_DEV, width), jnp.float32),
        jax.ShapeDtypeStruct((1, BINS_DEV), jnp.float32),
    )
    results = pl.pallas_call(
        exchange,
        out_shape=shapes,
        in_specs=[hbm] * 3,
        out_specs=(vmem, vmem),
        scratch_shapes=[
            pltpu.VMEM((goals, width), jnp.bfloat16),
            pltpu.VMEM((1, goals), jnp.int32),
            pltpu.VMEM((1, goals), jnp.float32),
            pltpu.VMEM((CHIPS, 2 * DEPTH, 2, width), jnp.bfloat16),
            pltpu.VMEM((PLANE, 2 * DEPTH, 2, width), jnp.bfloat16),
            pltpu.VMEM((DEPTH, PLANE, 2, width), jnp.bfloat16),
            pltpu.VMEM((2 * CHIPS, 128), jnp.float32),
            pltpu.VMEM((2 * PLANE, 128), jnp.float32),
            pltpu.VMEM((4 * DEPTH, 128), jnp.float32),
            pltpu.VMEM((2 * DEPTH, 128), jnp.float32),
            dma((3,)), dma(()), dma((4,)), dma(()), dma(()), dma(()), dma(()), dma(()), dma(()), dma(()),
            pltpu.SemaphoreType.REGULAR,
        ],
        compiler_params=pltpu.CompilerParams(collective_id=0, has_side_effects=True, vmem_limit_bytes=4 << 20),
        name="exchange",
    )(*[
        pltpu.with_memory_space_constraint(array, pltpu.HBM)
        for array in (goal_embed, goal_bins.reshape(1, goals), goal_weights.reshape(1, goals))
    ])
    mean, rarity = pl.pallas_call(
        write_out,
        out_shape=shapes,
        in_specs=[vmem, vmem],
        out_specs=(hbm, hbm),
        scratch_shapes=[dma((2,))],
        compiler_params=pltpu.CompilerParams(vmem_limit_bytes=1 << 20),
        name="write_out",
    )(*results)
    return mean, rarity[0]


def solution(mesh):
    flat = Mesh(mesh.devices.reshape(-1), (AXIS,))
    return jax.shard_map(
        shards, mesh=flat, in_specs=(P(AXIS, None), P(AXIS), P(AXIS)),
        out_specs=(P(AXIS, None), P(AXIS)), check_vma=False,
    )
```

```python
import functools

import jax
import jax.numpy as jnp
from jax import lax
from jax.experimental import pallas as pl
from jax.experimental.pallas import tpu as pltpu
from jax.sharding import Mesh
from jax.sharding import PartitionSpec as P

BINS_DEV = 64
AXIS = "device"
LOGICAL = pl.DeviceIdType.LOGICAL
DEVICES = 256
CHIPS = 16
PLANE = 32
DEPTH = 8
HOPS = (0, 1, 2, 1)
STEPS = sorted(range(1, CHIPS), key=lambda step: -(HOPS[step >> 2] + HOPS[step & 3]))
GROUPS = (0, 3, 1, 2)
FIRST = 1
FIRST_LOTS = pl.ds(0, 2 * FIRST)
REST_LOTS = pl.ds(2 * FIRST, 2 * (DEPTH - FIRST))


EARLIEST = 1
OPPOSITE = 4
BYPASSED = 129


def depth_of(flat):
    return ((flat >> 6) << 1) | ((flat >> 3) & 1)


def chip_of(flat):
    return (((flat >> 4) & 3) << 2) | ((flat >> 1) & 3)


def flat_of_chip(chip):
    return ((chip >> 2) << 4) | ((chip & 3) << 1)


def flat_of_depth(depth):
    return ((depth >> 1) << 6) | ((depth & 1) << 3)


def remote(src, dst, send, recv, target):
    return pltpu.make_async_remote_copy(
        src_ref=src, dst_ref=dst, send_sem=send, recv_sem=recv, device_id=target, device_id_type=LOGICAL
    )


def two(index):
    return pl.ds(pl.multiple_of(2 * index, 2), 2)


def turned_tags(tags_ref):
    plane = tags_ref[...]
    totals = jnp.broadcast_to(plane[:, 4 * DEPTH : 4 * DEPTH + 1], (2 * PLANE, 128))
    return jnp.transpose(jnp.concatenate([plane, totals], axis=0))


def exchange(
    embed_hbm, bins_hbm, weights_hbm, mean_ref, rarity_ref,
    embed, bins, weights, packed, relay, arrived, tags, plane_tags, direct_tags, column, depth_tags,
    in_sems, send_plane, recv_plane, recv_rest, send_depth, recv_depth,
    send_tags, recv_tags, send_column, recv_column, send_direct, recv_direct, send_rows, column_ready,
):
    me = lax.axis_index(AXIS)
    core = me & 1
    my_depth = depth_of(me)
    my_chip = chip_of(me)
    my_place = my_chip * 2 + core
    my_row = my_chip >> 2
    bottom = flat_of_chip(my_chip)
    loads = [
        pltpu.make_async_copy(bins_hbm, bins, in_sems.at[0]),
        pltpu.make_async_copy(weights_hbm, weights, in_sems.at[1]),
        pltpu.make_async_copy(embed_hbm, embed, in_sems.at[2]),
    ]
    for load in loads:
        load.start()
    barrier = pltpu.get_barrier_semaphore()

    def greet(target):
        pl.semaphore_signal(barrier, inc=1, device_id=target, device_id_type=LOGICAL)

    def other_relay(turn):
        return bottom | flat_of_depth(turn + (turn >= my_depth).astype(jnp.int32)) | 1

    greet(me ^ 1)

    @pl.when(core == 1)
    def _():
        for step in STEPS:
            greet(me ^ flat_of_chip(step))
            greet(me ^ flat_of_chip(step) ^ 1)
        for turn in range(DEPTH - 1):
            greet(other_relay(turn))

    @pl.when(me == EARLIEST)
    def _():
        for place in range(PLANE - 1, -1, -1):
            target = flat_of_depth(OPPOSITE) | flat_of_chip(place >> 1) | (place & 1)
            if target != BYPASSED:
                greet(target)

    is_opposite = (my_depth == OPPOSITE).astype(jnp.int32)

    for load in loads:
        load.wait()

    lanes = lax.broadcasted_iota(jnp.int32, (128, 128), 1)
    rows = lax.broadcasted_iota(jnp.int32, (128, 128), 0)
    bin_row = jnp.broadcast_to(bins[...], (128, 128))
    weight_row = jnp.broadcast_to(weights[...], (128, 128))
    bin_col = jnp.transpose(bin_row.astype(jnp.float32)).astype(jnp.int32)
    weight_col = jnp.transpose(weight_row)
    owner_row = bin_row >> 6
    owner_col = bin_col >> 6
    earlier = jnp.where((owner_row == owner_col) & (rows < lanes), 1.0, 0.0)
    slot_of = jnp.sum(earlier, axis=0, keepdims=True).astype(jnp.int32)
    owner = bins[...] >> 6
    row_id = ((chip_of(owner) * DEPTH + depth_of(owner)) * 2 + (owner & 1)) * 2 + slot_of
    tag_id = chip_of(owner) * 2 + slot_of

    lane_of = (depth_of(owner_col) * 2 + (owner_col & 1)) * 2
    offset_col = (bin_col & (BINS_DEV - 1)).astype(jnp.float32)
    values = jnp.where(lanes == lane_of, weight_col, 0.0) + jnp.where(lanes == lane_of + 1, offset_col, 0.0)
    tag_lanes = lax.broadcasted_iota(jnp.int32, (2 * CHIPS, 128), 1)
    tag_rows = lax.broadcasted_iota(jnp.int32, (2 * CHIPS, 128), 0)
    tag_pick = (tag_rows == tag_id).astype(jnp.float32)
    local_total = jnp.sum(weights[...])
    tags[...] = jnp.dot(
        tag_pick, values, precision=lax.Precision.HIGHEST, preferred_element_type=jnp.float32
    ) + jnp.where((tag_lanes == 4 * DEPTH) & (tag_rows % 2 == 0), local_total, 0.0)

    scaled = (weight_col * embed[...].astype(jnp.float32)).astype(jnp.bfloat16)
    pick = (lax.broadcasted_iota(jnp.int32, (2 * DEVICES, 128), 0) == row_id).astype(jnp.float32)
    packed.reshape(2 * DEVICES, 128)[...] = jnp.dot(
        pick.astype(jnp.bfloat16), scaled, preferred_element_type=jnp.float32
    ).astype(jnp.bfloat16)

    def hand_tags(chip, target):
        remote(tags.at[two(chip)], plane_tags.at[two(my_place)], send_tags, recv_tags, target).start()

    def hand_first(chip, target, group):
        remote(
            packed.at[chip, FIRST_LOTS], relay.at[my_place, FIRST_LOTS],
            send_plane, recv_plane.at[group], target,
        ).start()

    def hand_rest(chip, target):
        remote(
            packed.at[chip, REST_LOTS], relay.at[my_place, REST_LOTS], send_plane, recv_rest, target
        ).start()

    def hand_direct():
        remote(tags.at[two(0)], direct_tags.at[two(my_place)], send_direct, recv_direct, EARLIEST).start()
        remote(
            packed.at[0, EARLIEST], arrived.at[OPPOSITE, my_place], send_rows, recv_depth, EARLIEST
        ).start()

    def hand_all():
        pl.when(my_depth == OPPOSITE)(hand_direct)
        for step in STEPS:
            hand_tags(my_chip ^ step, (me ^ flat_of_chip(step)) | 1)
            hand_first(my_chip ^ step, (me ^ flat_of_chip(step)) | 1, step >> 2)

    everything = arrived.at[pl.ds(0, DEPTH)]
    all_tags = pl.ds(0, 2 * DEPTH)

    @pl.when(core == 0)
    def _():
        pl.semaphore_wait(barrier, CHIPS + is_opposite)
        hand_all()
        hand_tags(my_chip, me ^ 1)
        hand_first(my_chip, me ^ 1, 0)
        for step in STEPS:
            hand_rest(my_chip ^ step, (me ^ flat_of_chip(step)) | 1)
        hand_rest(my_chip, me ^ 1)
        remote(depth_tags.at[all_tags], depth_tags.at[all_tags], send_column, recv_column, me ^ 1).wait_recv()

    @pl.when(core == 1)
    def _():
        pl.semaphore_wait(barrier, CHIPS - 1 + DEPTH - 1 + 1 + jnp.where(me == BYPASSED, 0, is_opposite))
        hand_all()
        for step in STEPS:
            hand_rest(my_chip ^ step, (me ^ flat_of_chip(step)) | 1)
        for turn in range(DEPTH - 1):
            pl.semaphore_signal(column_ready, inc=1, device_id=other_relay(turn), device_id_type=LOGICAL)
        relay[my_place] = packed[my_chip]
        plane_tags[two(my_place)] = tags[two(my_chip)]
        pl.semaphore_wait(column_ready, DEPTH - 1)

        def both_cores(depths, send_to):
            for depth in depths:
                column_at = bottom | flat_of_depth(depth)
                send_to(column_at, 2 * depth)
                wanted = my_depth != depth
                if depth == 0:
                    wanted = wanted & (me != BYPASSED)
                pl.when(wanted)(functools.partial(send_to, column_at | 1, 2 * depth + 1))

        def pass_on(group):
            count = 8 if group else 7
            part = relay.at[pl.ds(0, count), FIRST_LOTS]
            remote(part, part, send_plane, recv_plane.at[group], me ^ 1).wait_recv()
            members = pl.ds(pl.multiple_of((my_row ^ group) * 8, 8), 8)

            def send_to(target, lot):
                remote(
                    relay.at[members, lot], arrived.at[my_depth, members], send_depth, recv_depth, target
                ).start()

            both_cores(range(FIRST), send_to)

        for group in GROUPS[:3]:
            pass_on(group)

        others = plane_tags.at[pl.ds(0, 2 * (PLANE - 1))]
        remote(others, others, send_tags, recv_tags, me ^ 1).wait_recv()
        column[...] = turned_tags(plane_tags)[: 4 * DEPTH]

        def send_column_to(target, lot):
            remote(
                column.at[two(lot)], depth_tags.at[two(my_depth)], send_column, recv_column, target
            ).start()

        both_cores(range(DEPTH), send_column_to)
        depth_tags[two(my_depth)] = column[two(my_depth * 2 + 1)]
        pass_on(GROUPS[3])
        part = relay.at[pl.ds(0, PLANE - 1), REST_LOTS]
        remote(part, part, send_plane, recv_rest, me ^ 1).wait_recv()

        def send_rest_to(target, lot):
            remote(relay.at[:, lot], arrived.at[my_depth], send_depth, recv_depth, target).start()

        both_cores(range(FIRST, DEPTH), send_rest_to)
        arrived[my_depth] = relay[:, my_depth * 2 + 1]

        @pl.when(me != EARLIEST)
        def _():
            most = depth_tags.at[pl.ds(0, 2 * (DEPTH - 1))]
            remote(most, most, send_column, recv_column, me ^ 1).wait_recv()

        @pl.when(me == EARLIEST)
        def _():
            remote(direct_tags, direct_tags, send_direct, recv_direct, me ^ 1).wait_recv()
            turned = turned_tags(direct_tags)
            most = depth_tags.at[pl.ds(0, 2 * (DEPTH - 2))]
            remote(most, most, send_column, recv_column, me ^ 1).wait_recv()
            depth_tags[two(OPPOSITE)] = turned[2 * EARLIEST : 2 * EARLIEST + 2]

    half = lax.broadcasted_iota(jnp.int32, (1, 128), 1) < 64
    labels = lax.broadcasted_iota(jnp.int32, (BINS_DEV, 128), 0).astype(jnp.float32)
    totals = jnp.zeros((1, 128), jnp.float32)
    weighed = jnp.zeros((BINS_DEV, 128), jnp.float32)
    selectors = []
    for pair in range(DEPTH // 2):
        first = depth_tags[4 * pair : 4 * pair + 2]
        second = depth_tags[4 * pair + 2 : 4 * pair + 4]
        totals = totals + first[0:1] + second[0:1]
        turned = pltpu.roll(second, 64, axis=1)
        weight = jnp.where(half, first[0:1], turned[0:1])
        offset = jnp.where(half, first[1:2], turned[1:2])
        chosen = labels == offset
        weighed = weighed + jnp.where(chosen, weight, 0.0)
        selectors.append(jnp.where(chosen, 1.0, 0.0).astype(jnp.bfloat16))
    den = jnp.broadcast_to(jnp.sum(weighed, axis=1, keepdims=True), (BINS_DEV, 128)) + 1.0
    total = jnp.sum(jnp.where(half, 0.0, totals), axis=1, keepdims=True)
    rarity_ref[...] = jnp.log(total / (BINS_DEV * DEVICES)) - jnp.log(jnp.transpose(den)[0:1, :BINS_DEV])

    @pl.when(core == 0)
    def _():
        remote(everything, everything, send_depth, recv_depth, me ^ 1).wait_recv()

    @pl.when(core == 1)
    def _():
        most = arrived.at[pl.ds(0, DEPTH - 1)]
        remote(most, most, send_depth, recv_depth, me ^ 1).wait_recv()

    mean_ref[...] = jnp.dot(
        jnp.concatenate(selectors, axis=1), arrived.reshape(2 * DEVICES, 128)[...],
        preferred_element_type=jnp.float32,
    ) / den

    def sent(chips):
        part = packed.at[pl.ds(0, chips)]
        remote(part, part, send_plane, recv_plane.at[0], me ^ 1).wait_send()
        part = tags.at[pl.ds(0, 2 * chips)]
        remote(part, part, send_tags, recv_tags, me ^ 1).wait_send()

    @pl.when(core == 0)
    def _():
        sent(CHIPS)

    @pl.when(core == 1)
    def _():
        sent(CHIPS - 1)

    def relayed(targets):
        part = relay.at[pl.ds(0, 2 * targets)]
        remote(part, part, send_depth, recv_depth, me ^ 1).wait_send()
        part = column.at[pl.ds(0, 2 * targets)]
        remote(part, part, send_column, recv_column, me ^ 1).wait_send()

    pl.when((core == 1) & (me != BYPASSED))(functools.partial(relayed, 2 * DEPTH - 1))
    pl.when(me == BYPASSED)(functools.partial(relayed, 2 * DEPTH - 2))

    @pl.when(my_depth == OPPOSITE)
    def _():
        part = tags.at[two(0)]
        remote(part, part, send_direct, recv_direct, me ^ 1).wait_send()
        part = packed.at[0, EARLIEST]
        remote(part, part, send_rows, recv_depth, me ^ 1).wait_send()


def write_out(mean, rarity, mean_hbm, rarity_hbm, sems):
    copies = [
        pltpu.make_async_copy(mean, mean_hbm, sems.at[0]),
        pltpu.make_async_copy(rarity, rarity_hbm, sems.at[1]),
    ]
    for copy in copies:
        copy.start()
    for copy in copies:
        copy.wait()


def shards(goal_embed, goal_bins, goal_weights):
    width = goal_embed.shape[1]
    goals = goal_embed.shape[0]
    vmem = pl.BlockSpec(memory_space=pltpu.VMEM)
    hbm = pl.BlockSpec(memory_space=pltpu.HBM)
    dma = pltpu.SemaphoreType.DMA
    shapes = (
        jax.ShapeDtypeStruct((BINS_DEV, width), jnp.float32),
        jax.ShapeDtypeStruct((1, BINS_DEV), jnp.float32),
    )
    results = pl.pallas_call(
        exchange,
        out_shape=shapes,
        in_specs=[hbm] * 3,
        out_specs=(vmem, vmem),
        scratch_shapes=[
            pltpu.VMEM((goals, width), jnp.bfloat16),
            pltpu.VMEM((1, goals), jnp.int32),
            pltpu.VMEM((1, goals), jnp.float32),
            pltpu.VMEM((CHIPS, 2 * DEPTH, 2, width), jnp.bfloat16),
            pltpu.VMEM((PLANE, 2 * DEPTH, 2, width), jnp.bfloat16),
            pltpu.VMEM((DEPTH, PLANE, 2, width), jnp.bfloat16),
            pltpu.VMEM((2 * CHIPS, 128), jnp.float32),
            pltpu.VMEM((2 * PLANE, 128), jnp.float32),
            pltpu.VMEM((2 * PLANE, 128), jnp.float32),
            pltpu.VMEM((4 * DEPTH, 128), jnp.float32),
            pltpu.VMEM((2 * DEPTH, 128), jnp.float32),
            dma((3,)), dma(()), dma((4,)), dma(()), dma(()), dma(()), dma(()), dma(()), dma(()), dma(()),
            dma(()), dma(()), dma(()),
            pltpu.SemaphoreType.REGULAR,
        ],
        compiler_params=pltpu.CompilerParams(collective_id=0, has_side_effects=True, vmem_limit_bytes=4 << 20),
        name="exchange",
    )(*[
        pltpu.with_memory_space_constraint(array, pltpu.HBM)
        for array in (goal_embed, goal_bins.reshape(1, goals), goal_weights.reshape(1, goals))
    ])
    mean, rarity = pl.pallas_call(
        write_out,
        out_shape=shapes,
        in_specs=[vmem, vmem],
        out_specs=(hbm, hbm),
        scratch_shapes=[dma((2,))],
        compiler_params=pltpu.CompilerParams(vmem_limit_bytes=1 << 20),
        name="write_out",
    )(*results)
    return mean, rarity[0]


def solution(mesh):
    flat = Mesh(mesh.devices.reshape(-1), (AXIS,))
    return jax.shard_map(
        shards, mesh=flat, in_specs=(P(AXIS, None), P(AXIS), P(AXIS)),
        out_specs=(P(AXIS, None), P(AXIS)), check_vma=False,
    )
```

```python
import functools

import jax
import jax.numpy as jnp
from jax import lax
from jax.experimental import pallas as pl
from jax.experimental.pallas import tpu as pltpu
from jax.sharding import Mesh
from jax.sharding import PartitionSpec as P

BINS_DEV = 64
AXIS = "device"
LOGICAL = pl.DeviceIdType.LOGICAL
DEVICES = 256
CHIPS = 16
PLANE = 32
DEPTH = 8
HOPS = (0, 1, 2, 1)
STEPS = sorted(range(1, CHIPS), key=lambda step: -(HOPS[step >> 2] + HOPS[step & 3]))
GROUPS = (0, 3, 1, 2)
FIRST_LOTS = pl.ds(0, 2)
TIERS = ((1, 3), (3, 8))


def lots_of(tier):
    return pl.ds(2 * tier[0], 2 * (tier[1] - tier[0]))


LATE = 4
EARLIEST = 1
DIRECT = (4, 5)
BYPASSED = (129, 137)


def depth_of(flat):
    return ((flat >> 6) << 1) | ((flat >> 3) & 1)


def chip_of(flat):
    return (((flat >> 4) & 3) << 2) | ((flat >> 1) & 3)


def flat_of_chip(chip):
    return ((chip >> 2) << 4) | ((chip & 3) << 1)


def flat_of_depth(depth):
    return ((depth >> 1) << 6) | ((depth & 1) << 3)


def remote(src, dst, send, recv, target):
    return pltpu.make_async_remote_copy(
        src_ref=src, dst_ref=dst, send_sem=send, recv_sem=recv, device_id=target, device_id_type=LOGICAL
    )


def two(index):
    return pl.ds(pl.multiple_of(2 * index, 2), 2)


def turned_tags(tags_ref):
    plane = tags_ref[...]
    totals = jnp.broadcast_to(plane[:, 4 * DEPTH : 4 * DEPTH + 1], (2 * PLANE, 128))
    return jnp.transpose(jnp.concatenate([plane, totals], axis=0))


def exchange(
    embed_hbm, bins_hbm, weights_hbm, mean_ref, rarity_ref,
    embed, bins, weights, packed, relay, arrived, tags, plane_tags, direct_tags, column, depth_tags,
    in_sems, send_plane, recv_plane, recv_rest, send_depth, recv_depth,
    send_tags, recv_tags, send_column, recv_column, send_direct, recv_direct, send_rows, above_ready, below_ready,
):
    me = lax.axis_index(AXIS)
    core = me & 1
    my_depth = depth_of(me)
    my_chip = chip_of(me)
    my_place = my_chip * 2 + core
    my_row = my_chip >> 2
    bottom = flat_of_chip(my_chip)
    loads = [
        pltpu.make_async_copy(bins_hbm, bins, in_sems.at[0]),
        pltpu.make_async_copy(weights_hbm, weights, in_sems.at[1]),
        pltpu.make_async_copy(embed_hbm, embed, in_sems.at[2]),
    ]
    for load in loads:
        load.start()
    barrier = pltpu.get_barrier_semaphore()

    def greet(target):
        pl.semaphore_signal(barrier, inc=1, device_id=target, device_id_type=LOGICAL)

    def relays(first, last, act):
        def visit(depth, carry):
            act(bottom | flat_of_depth(depth) | 1)
            return carry

        lax.fori_loop(first, last, visit, 0)

    greet(me ^ 1)

    @pl.when(core == 1)
    def _():
        for step in STEPS:
            greet(me ^ flat_of_chip(step))
            greet(me ^ flat_of_chip(step) ^ 1)

    @pl.when((core == 1) | (my_depth < LATE))
    def _():
        relays(my_depth + 1, DEPTH, greet)

    @pl.when(me == EARLIEST)
    def _():
        for place in range(PLANE - 1, -1, -1):
            for depth in DIRECT:
                target = flat_of_depth(depth) | flat_of_chip(place >> 1) | (place & 1)
                if target not in BYPASSED:
                    greet(target)

    is_direct = (my_depth == DIRECT[0]) | (my_depth == DIRECT[1])
    bypassed = (me == BYPASSED[0]) | (me == BYPASSED[1])
    one_more = is_direct.astype(jnp.int32)

    for load in loads:
        load.wait()

    lanes = lax.broadcasted_iota(jnp.int32, (128, 128), 1)
    rows = lax.broadcasted_iota(jnp.int32, (128, 128), 0)
    bin_row = jnp.broadcast_to(bins[...], (128, 128))
    weight_row = jnp.broadcast_to(weights[...], (128, 128))
    bin_col = jnp.transpose(bin_row.astype(jnp.float32)).astype(jnp.int32)
    weight_col = jnp.transpose(weight_row)
    owner_row = bin_row >> 6
    owner_col = bin_col >> 6
    earlier = jnp.where((owner_row == owner_col) & (rows < lanes), 1.0, 0.0)
    slot_of = jnp.sum(earlier, axis=0, keepdims=True).astype(jnp.int32)
    owner = bins[...] >> 6
    row_id = ((chip_of(owner) * DEPTH + depth_of(owner)) * 2 + (owner & 1)) * 2 + slot_of
    tag_id = chip_of(owner) * 2 + slot_of

    lane_of = (depth_of(owner_col) * 2 + (owner_col & 1)) * 2
    offset_col = (bin_col & (BINS_DEV - 1)).astype(jnp.float32)
    values = jnp.where(lanes == lane_of, weight_col, 0.0) + jnp.where(lanes == lane_of + 1, offset_col, 0.0)
    tag_lanes = lax.broadcasted_iota(jnp.int32, (2 * CHIPS, 128), 1)
    tag_rows = lax.broadcasted_iota(jnp.int32, (2 * CHIPS, 128), 0)
    tag_pick = (tag_rows == tag_id).astype(jnp.float32)
    local_total = jnp.sum(weights[...])
    tags[...] = jnp.dot(
        tag_pick, values, precision=lax.Precision.HIGHEST, preferred_element_type=jnp.float32
    ) + jnp.where((tag_lanes == 4 * DEPTH) & (tag_rows % 2 == 0), local_total, 0.0)

    scaled = (weight_col * embed[...].astype(jnp.float32)).astype(jnp.bfloat16)
    pick = (lax.broadcasted_iota(jnp.int32, (2 * DEVICES, 128), 0) == row_id).astype(jnp.float32)
    packed.reshape(2 * DEVICES, 128)[...] = jnp.dot(
        pick.astype(jnp.bfloat16), scaled, preferred_element_type=jnp.float32
    ).astype(jnp.bfloat16)

    def hand_tags(chip, target):
        remote(tags.at[two(chip)], plane_tags.at[two(my_place)], send_tags, recv_tags, target).start()

    def hand_first(chip, target, group):
        remote(
            packed.at[chip, FIRST_LOTS], relay.at[my_place, FIRST_LOTS],
            send_plane, recv_plane.at[group], target,
        ).start()

    def hand_tier(index, chip, target):
        lots = lots_of(TIERS[index])
        remote(
            packed.at[chip, lots], relay.at[my_place, lots], send_plane, recv_rest.at[index], target
        ).start()

    def hand_direct():
        row = (my_depth - DIRECT[0]) * PLANE + my_place
        remote(tags.at[two(0)], direct_tags.at[two(row)], send_direct, recv_direct, EARLIEST).start()
        remote(
            packed.at[0, EARLIEST], arrived.at[my_depth, my_place], send_rows, recv_depth, EARLIEST
        ).start()

    def hand_all():
        pl.when(is_direct)(hand_direct)
        for step in STEPS:
            hand_tags(my_chip ^ step, (me ^ flat_of_chip(step)) | 1)
            hand_first(my_chip ^ step, (me ^ flat_of_chip(step)) | 1, step >> 2)

    everything = arrived.at[pl.ds(0, DEPTH)]
    all_tags = pl.ds(0, 2 * DEPTH)

    @pl.when(core == 0)
    def _():
        pl.semaphore_wait(barrier, CHIPS + one_more)
        hand_all()
        hand_tags(my_chip, me ^ 1)
        hand_first(my_chip, me ^ 1, 0)
        for index in range(len(TIERS)):
            for step in STEPS:
                hand_tier(index, my_chip ^ step, (me ^ flat_of_chip(step)) | 1)
            hand_tier(index, my_chip, me ^ 1)
        remote(depth_tags.at[all_tags], depth_tags.at[all_tags], send_column, recv_column, me ^ 1).wait_recv()

    @pl.when(core == 1)
    def _():
        greeted = my_depth + jnp.minimum(my_depth, LATE) + jnp.where(bypassed, 0, one_more)
        pl.semaphore_wait(barrier, CHIPS + greeted)
        hand_all()

        def answer(target):
            pl.semaphore_signal(above_ready, inc=1, device_id=target, device_id_type=LOGICAL)

        relays(0, my_depth, answer)
        for index in range(len(TIERS)):
            for step in STEPS:
                hand_tier(index, my_chip ^ step, (me ^ flat_of_chip(step)) | 1)
        relay[my_place] = packed[my_chip]
        plane_tags[two(my_place)] = tags[two(my_chip)]

        @pl.when((my_depth >= LATE) & (my_depth < DEPTH - 1))
        def _():
            pl.semaphore_wait(above_ready, DEPTH - 1 - my_depth)

            def answer_late(target):
                pl.semaphore_signal(below_ready, inc=1, device_id=target, device_id_type=LOGICAL)

            relays(my_depth + 1, DEPTH, answer_late)

        def await_column():
            @pl.when(my_depth > LATE)
            def _():
                pl.semaphore_wait(below_ready, my_depth - LATE)

            @pl.when(my_depth < LATE)
            def _():
                pl.semaphore_wait(above_ready, DEPTH - 1 - my_depth)

        def both_cores(depths, send_to, only=None):
            for depth in depths:
                column_at = bottom | flat_of_depth(depth)
                wanted = my_depth != depth
                if only is None:
                    send_to(column_at, 2 * depth)
                else:
                    chosen = only(depth)
                    pl.when(chosen)(functools.partial(send_to, column_at, 2 * depth))
                    wanted = wanted & chosen
                if depth == 0:
                    wanted = wanted & jnp.logical_not(bypassed)
                pl.when(wanted)(functools.partial(send_to, column_at | 1, 2 * depth + 1))

        def pass_on(group):
            count = 8 if group else 7
            part = relay.at[pl.ds(0, count), FIRST_LOTS]
            remote(part, part, send_plane, recv_plane.at[group], me ^ 1).wait_recv()
            members = pl.ds(pl.multiple_of((my_row ^ group) * 8, 8), 8)

            def send_to(target, lot):
                remote(
                    relay.at[members, lot], arrived.at[my_depth, members], send_depth, recv_depth, target
                ).start()

            both_cores(range(1), send_to)

        for group in GROUPS[:3]:
            pass_on(group)

        others = plane_tags.at[pl.ds(0, 2 * (PLANE - 1))]
        remote(others, others, send_tags, recv_tags, me ^ 1).wait_recv()
        column[...] = turned_tags(plane_tags)[: 4 * DEPTH]

        def send_column_to(target, lot):
            remote(
                column.at[two(lot)], depth_tags.at[two(my_depth)], send_column, recv_column, target
            ).start()

        both_cores(range(1), send_column_to)
        both_cores(range(1, LATE), send_column_to, lambda depth: my_depth >= depth)
        depth_tags[two(my_depth)] = column[two(my_depth * 2 + 1)]
        pass_on(GROUPS[3])
        await_column()
        both_cores(range(1, LATE), send_column_to, lambda depth: my_depth < depth)
        both_cores(range(LATE, DEPTH), send_column_to)

        def send_rest_to(target, lot):
            remote(relay.at[:, lot], arrived.at[my_depth], send_depth, recv_depth, target).start()

        for index, tier in enumerate(TIERS):
            part = relay.at[pl.ds(0, PLANE - 1), lots_of(tier)]
            remote(part, part, send_plane, recv_rest.at[index], me ^ 1).wait_recv()
            both_cores(range(*tier), send_rest_to)
        arrived[my_depth] = relay[:, my_depth * 2 + 1]

        @pl.when(me != EARLIEST)
        def _():
            most = depth_tags.at[pl.ds(0, 2 * (DEPTH - 1))]
            remote(most, most, send_column, recv_column, me ^ 1).wait_recv()

        @pl.when(me == EARLIEST)
        def _():
            remote(direct_tags, direct_tags, send_direct, recv_direct, me ^ 1).wait_recv()
            turned = jnp.transpose(direct_tags[...])
            pair = turned[2 * EARLIEST : 2 * EARLIEST + 2]
            totals = jnp.broadcast_to(turned[4 * DEPTH : 4 * DEPTH + 1], (2, 128))
            lower = lax.broadcasted_iota(jnp.int32, (2, 128), 1) < 64
            depth_tags[2 * DIRECT[0] : 2 * DIRECT[0] + 2] = jnp.where(
                lower, pair, pltpu.roll(totals, 64, axis=1)
            )
            depth_tags[2 * DIRECT[1] : 2 * DIRECT[1] + 2] = jnp.where(
                lower, pltpu.roll(pair, 64, axis=1), totals
            )
            most = depth_tags.at[pl.ds(0, 2 * (DEPTH - 1 - len(DIRECT)))]
            remote(most, most, send_column, recv_column, me ^ 1).wait_recv()

    half = lax.broadcasted_iota(jnp.int32, (1, 128), 1) < 64
    labels = lax.broadcasted_iota(jnp.int32, (BINS_DEV, 128), 0).astype(jnp.float32)
    totals = jnp.zeros((1, 128), jnp.float32)
    weighed = jnp.zeros((BINS_DEV, 128), jnp.float32)
    selectors = []
    for pair in range(DEPTH // 2):
        first = depth_tags[4 * pair : 4 * pair + 2]
        second = depth_tags[4 * pair + 2 : 4 * pair + 4]
        totals = totals + first[0:1] + second[0:1]
        turned = pltpu.roll(second, 64, axis=1)
        weight = jnp.where(half, first[0:1], turned[0:1])
        offset = jnp.where(half, first[1:2], turned[1:2])
        chosen = labels == offset
        weighed = weighed + jnp.where(chosen, weight, 0.0)
        selectors.append(jnp.where(chosen, 1.0, 0.0).astype(jnp.bfloat16))
    @pl.when(core == 0)
    def _():
        remote(everything, everything, send_depth, recv_depth, me ^ 1).wait_recv()

    @pl.when(core == 1)
    def _():
        most = arrived.at[pl.ds(0, DEPTH - 1)]
        remote(most, most, send_depth, recv_depth, me ^ 1).wait_recv()

    den = jnp.broadcast_to(jnp.sum(weighed, axis=1, keepdims=True), (BINS_DEV, 128)) + 1.0
    total = jnp.sum(jnp.where(half, 0.0, totals), axis=1, keepdims=True)
    rarity_ref[...] = jnp.log(total / (BINS_DEV * DEVICES)) - jnp.log(jnp.transpose(den)[0:1, :BINS_DEV])

    mean_ref[...] = jnp.dot(
        jnp.concatenate(selectors, axis=1), arrived.reshape(2 * DEVICES, 128)[...],
        preferred_element_type=jnp.float32,
    ) / den

    def sent(chips):
        part = packed.at[pl.ds(0, chips)]
        remote(part, part, send_plane, recv_plane.at[0], me ^ 1).wait_send()
        part = tags.at[pl.ds(0, 2 * chips)]
        remote(part, part, send_tags, recv_tags, me ^ 1).wait_send()

    @pl.when(core == 0)
    def _():
        sent(CHIPS)

    @pl.when(core == 1)
    def _():
        sent(CHIPS - 1)

    def relayed(targets):
        part = relay.at[pl.ds(0, 2 * targets)]
        remote(part, part, send_depth, recv_depth, me ^ 1).wait_send()
        part = column.at[pl.ds(0, 2 * targets)]
        remote(part, part, send_column, recv_column, me ^ 1).wait_send()

    pl.when((core == 1) & jnp.logical_not(bypassed))(functools.partial(relayed, 2 * DEPTH - 1))
    pl.when(bypassed)(functools.partial(relayed, 2 * DEPTH - 2))

    @pl.when(is_direct)
    def _():
        part = tags.at[two(0)]
        remote(part, part, send_direct, recv_direct, me ^ 1).wait_send()
        part = packed.at[0, EARLIEST]
        remote(part, part, send_rows, recv_depth, me ^ 1).wait_send()


def write_out(mean, rarity, mean_hbm, rarity_hbm, sems):
    copies = [
        pltpu.make_async_copy(mean, mean_hbm, sems.at[0]),
        pltpu.make_async_copy(rarity, rarity_hbm, sems.at[1]),
    ]
    for copy in copies:
        copy.start()
    for copy in copies:
        copy.wait()


def shards(goal_embed, goal_bins, goal_weights):
    width = goal_embed.shape[1]
    goals = goal_embed.shape[0]
    vmem = pl.BlockSpec(memory_space=pltpu.VMEM)
    hbm = pl.BlockSpec(memory_space=pltpu.HBM)
    dma = pltpu.SemaphoreType.DMA
    shapes = (
        jax.ShapeDtypeStruct((BINS_DEV, width), jnp.float32),
        jax.ShapeDtypeStruct((1, BINS_DEV), jnp.float32),
    )
    results = pl.pallas_call(
        exchange,
        out_shape=shapes,
        in_specs=[hbm] * 3,
        out_specs=(vmem, vmem),
        scratch_shapes=[
            pltpu.VMEM((goals, width), jnp.bfloat16),
            pltpu.VMEM((1, goals), jnp.int32),
            pltpu.VMEM((1, goals), jnp.float32),
            pltpu.VMEM((CHIPS, 2 * DEPTH, 2, width), jnp.bfloat16),
            pltpu.VMEM((PLANE, 2 * DEPTH, 2, width), jnp.bfloat16),
            pltpu.VMEM((DEPTH, PLANE, 2, width), jnp.bfloat16),
            pltpu.VMEM((2 * CHIPS, 128), jnp.float32),
            pltpu.VMEM((2 * PLANE, 128), jnp.float32),
            pltpu.VMEM((2 * len(DIRECT) * PLANE, 128), jnp.float32),
            pltpu.VMEM((4 * DEPTH, 128), jnp.float32),
            pltpu.VMEM((2 * DEPTH, 128), jnp.float32),
            dma((3,)), dma(()), dma((4,)), dma((len(TIERS),)), dma(()), dma(()), dma(()), dma(()), dma(()), dma(()),
            dma(()), dma(()), dma(()),
            pltpu.SemaphoreType.REGULAR, pltpu.SemaphoreType.REGULAR,
        ],
        compiler_params=pltpu.CompilerParams(collective_id=0, has_side_effects=True, vmem_limit_bytes=4 << 20),
        name="exchange",
    )(*[
        pltpu.with_memory_space_constraint(array, pltpu.HBM)
        for array in (goal_embed, goal_bins.reshape(1, goals), goal_weights.reshape(1, goals))
    ])
    mean, rarity = pl.pallas_call(
        write_out,
        out_shape=shapes,
        in_specs=[vmem, vmem],
        out_specs=(hbm, hbm),
        scratch_shapes=[dma((2,))],
        compiler_params=pltpu.CompilerParams(vmem_limit_bytes=1 << 20),
        name="write_out",
    )(*results)
    return mean, rarity[0]


def solution(mesh):
    flat = Mesh(mesh.devices.reshape(-1), (AXIS,))
    return jax.shard_map(
        shards, mesh=flat, in_specs=(P(AXIS, None), P(AXIS), P(AXIS)),
        out_specs=(P(AXIS, None), P(AXIS)), check_vma=False,
    )
```

```python
import functools

import jax
import jax.numpy as jnp
from jax import lax
from jax.experimental import pallas as pl
from jax.experimental.pallas import tpu as pltpu
from jax.sharding import Mesh
from jax.sharding import PartitionSpec as P

BINS_DEV = 64
AXIS = "device"
LOGICAL = pl.DeviceIdType.LOGICAL
DEVICES = 256
CHIPS = 16
PLANE = 32
DEPTH = 8
HOPS = (0, 1, 2, 1)
STEPS = sorted(range(1, CHIPS), key=lambda step: -(HOPS[step >> 2] + HOPS[step & 3]))
GROUPS = (0, 3, 1, 2)
FIRST_LOTS = pl.ds(0, 2)
TIERS = ((1, 3), (3, 8))


def lots_of(tier):
    return pl.ds(2 * tier[0], 2 * (tier[1] - tier[0]))


LATE = 4
EARLIEST = 1
DIRECT = (4, 5, 6)
BYPASSED = (129, 137, 193)


def depth_of(flat):
    return ((flat >> 6) << 1) | ((flat >> 3) & 1)


def chip_of(flat):
    return (((flat >> 4) & 3) << 2) | ((flat >> 1) & 3)


def flat_of_chip(chip):
    return ((chip >> 2) << 4) | ((chip & 3) << 1)


def flat_of_depth(depth):
    return ((depth >> 1) << 6) | ((depth & 1) << 3)


def remote(src, dst, send, recv, target):
    return pltpu.make_async_remote_copy(
        src_ref=src, dst_ref=dst, send_sem=send, recv_sem=recv, device_id=target, device_id_type=LOGICAL
    )


def two(index):
    return pl.ds(pl.multiple_of(2 * index, 2), 2)


def turned_tags(tags_ref):
    plane = tags_ref[...]
    totals = jnp.broadcast_to(plane[:, 4 * DEPTH : 4 * DEPTH + 1], (2 * PLANE, 128))
    return jnp.transpose(jnp.concatenate([plane, totals], axis=0))


def exchange(
    embed_hbm, bins_hbm, weights_hbm, mean_ref, rarity_ref,
    embed, bins, weights, packed, relay, arrived, tags, plane_tags, direct_tags, column, depth_tags,
    in_sems, send_plane, recv_plane, recv_rest, send_depth, recv_depth,
    send_tags, recv_tags, send_column, recv_column, send_direct, recv_direct, send_rows, above_ready, below_ready,
):
    me = lax.axis_index(AXIS)
    core = me & 1
    my_depth = depth_of(me)
    my_chip = chip_of(me)
    my_place = my_chip * 2 + core
    my_row = my_chip >> 2
    bottom = flat_of_chip(my_chip)
    loads = [
        pltpu.make_async_copy(bins_hbm, bins, in_sems.at[0]),
        pltpu.make_async_copy(weights_hbm, weights, in_sems.at[1]),
        pltpu.make_async_copy(embed_hbm, embed, in_sems.at[2]),
    ]
    for load in loads:
        load.start()
    barrier = pltpu.get_barrier_semaphore()

    def greet(target):
        pl.semaphore_signal(barrier, inc=1, device_id=target, device_id_type=LOGICAL)

    def relays(first, last, act):
        def visit(depth, carry):
            act(bottom | flat_of_depth(depth) | 1)
            return carry

        lax.fori_loop(first, last, visit, 0)

    greet(me ^ 1)

    @pl.when(core == 1)
    def _():
        for step in STEPS:
            greet(me ^ flat_of_chip(step))
            greet(me ^ flat_of_chip(step) ^ 1)

    @pl.when((core == 1) | (my_depth < LATE))
    def _():
        relays(my_depth + 1, DEPTH, greet)

    @pl.when(me == EARLIEST)
    def _():
        for place in range(PLANE - 1, -1, -1):
            for depth in DIRECT:
                target = flat_of_depth(depth) | flat_of_chip(place >> 1) | (place & 1)
                if target not in BYPASSED:
                    greet(target)

    is_direct = (my_depth >= DIRECT[0]) & (my_depth <= DIRECT[-1])
    bypassed = is_direct & (my_chip == 0) & (core == 1)
    one_more = is_direct.astype(jnp.int32)

    for load in loads:
        load.wait()

    lanes = lax.broadcasted_iota(jnp.int32, (128, 128), 1)
    rows = lax.broadcasted_iota(jnp.int32, (128, 128), 0)
    bin_row = jnp.broadcast_to(bins[...], (128, 128))
    weight_row = jnp.broadcast_to(weights[...], (128, 128))
    bin_col = jnp.transpose(bin_row.astype(jnp.float32)).astype(jnp.int32)
    weight_col = jnp.transpose(weight_row)
    owner_row = bin_row >> 6
    owner_col = bin_col >> 6
    earlier = jnp.where((owner_row == owner_col) & (rows < lanes), 1.0, 0.0)
    slot_of = jnp.sum(earlier, axis=0, keepdims=True).astype(jnp.int32)
    owner = bins[...] >> 6
    row_id = ((chip_of(owner) * DEPTH + depth_of(owner)) * 2 + (owner & 1)) * 2 + slot_of
    tag_id = chip_of(owner) * 2 + slot_of

    lane_of = (depth_of(owner_col) * 2 + (owner_col & 1)) * 2
    offset_col = (bin_col & (BINS_DEV - 1)).astype(jnp.float32)
    values = jnp.where(lanes == lane_of, weight_col, 0.0) + jnp.where(lanes == lane_of + 1, offset_col, 0.0)
    tag_lanes = lax.broadcasted_iota(jnp.int32, (2 * CHIPS, 128), 1)
    tag_rows = lax.broadcasted_iota(jnp.int32, (2 * CHIPS, 128), 0)
    tag_pick = (tag_rows == tag_id).astype(jnp.float32)
    local_total = jnp.sum(weights[...])
    tags[...] = jnp.dot(
        tag_pick, values, precision=lax.Precision.HIGHEST, preferred_element_type=jnp.float32
    ) + jnp.where((tag_lanes == 4 * DEPTH) & (tag_rows % 2 == 0), local_total, 0.0)

    scaled = (weight_col * embed[...].astype(jnp.float32)).astype(jnp.bfloat16)
    pick = (lax.broadcasted_iota(jnp.int32, (2 * DEVICES, 128), 0) == row_id).astype(jnp.float32)
    packed.reshape(2 * DEVICES, 128)[...] = jnp.dot(
        pick.astype(jnp.bfloat16), scaled, preferred_element_type=jnp.float32
    ).astype(jnp.bfloat16)

    def hand_tags(chip, target):
        remote(tags.at[two(chip)], plane_tags.at[two(my_place)], send_tags, recv_tags, target).start()

    def hand_first(chip, target, group):
        remote(
            packed.at[chip, FIRST_LOTS], relay.at[my_place, FIRST_LOTS],
            send_plane, recv_plane.at[group], target,
        ).start()

    def hand_tier(index, chip, target):
        lots = lots_of(TIERS[index])
        remote(
            packed.at[chip, lots], relay.at[my_place, lots], send_plane, recv_rest.at[index], target
        ).start()

    def hand_direct():
        row = (my_depth - DIRECT[0]) * PLANE + my_place
        remote(tags.at[two(0)], direct_tags.at[two(row)], send_direct, recv_direct, EARLIEST).start()
        remote(
            packed.at[0, EARLIEST], arrived.at[my_depth, my_place], send_rows, recv_depth, EARLIEST
        ).start()

    def hand_all():
        pl.when(is_direct)(hand_direct)
        for step in STEPS:
            hand_tags(my_chip ^ step, (me ^ flat_of_chip(step)) | 1)
            hand_first(my_chip ^ step, (me ^ flat_of_chip(step)) | 1, step >> 2)

    everything = arrived.at[pl.ds(0, DEPTH)]
    all_tags = pl.ds(0, 2 * DEPTH)

    @pl.when(core == 0)
    def _():
        pl.semaphore_wait(barrier, CHIPS + one_more)
        hand_all()
        hand_tags(my_chip, me ^ 1)
        hand_first(my_chip, me ^ 1, 0)
        for index in range(len(TIERS)):
            for step in STEPS:
                hand_tier(index, my_chip ^ step, (me ^ flat_of_chip(step)) | 1)
            hand_tier(index, my_chip, me ^ 1)
        remote(depth_tags.at[all_tags], depth_tags.at[all_tags], send_column, recv_column, me ^ 1).wait_recv()

    @pl.when(core == 1)
    def _():
        greeted = my_depth + jnp.minimum(my_depth, LATE) + jnp.where(bypassed, 0, one_more)
        pl.semaphore_wait(barrier, CHIPS + greeted)
        hand_all()

        def answer(target):
            pl.semaphore_signal(above_ready, inc=1, device_id=target, device_id_type=LOGICAL)

        relays(0, my_depth, answer)
        for index in range(len(TIERS)):
            for step in STEPS:
                hand_tier(index, my_chip ^ step, (me ^ flat_of_chip(step)) | 1)
        relay[my_place] = packed[my_chip]
        plane_tags[two(my_place)] = tags[two(my_chip)]

        @pl.when((my_depth >= LATE) & (my_depth < DEPTH - 1))
        def _():
            pl.semaphore_wait(above_ready, DEPTH - 1 - my_depth)

            def answer_late(target):
                pl.semaphore_signal(below_ready, inc=1, device_id=target, device_id_type=LOGICAL)

            relays(my_depth + 1, DEPTH, answer_late)

        def await_column():
            @pl.when(my_depth > LATE)
            def _():
                pl.semaphore_wait(below_ready, my_depth - LATE)

            @pl.when(my_depth < LATE)
            def _():
                pl.semaphore_wait(above_ready, DEPTH - 1 - my_depth)

        def both_cores(depths, send_to, only=None):
            for depth in depths:
                column_at = bottom | flat_of_depth(depth)
                wanted = my_depth != depth
                chosen = True if only is None else only(depth)
                if only is not None:
                    wanted = wanted & chosen
                if depth == 0:
                    wanted = wanted & jnp.logical_not(bypassed)
                pl.when(wanted)(functools.partial(send_to, column_at | 1, 2 * depth + 1))
                if only is None:
                    send_to(column_at, 2 * depth)
                else:
                    pl.when(chosen)(functools.partial(send_to, column_at, 2 * depth))

        def pass_on(group):
            count = 8 if group else 7
            part = relay.at[pl.ds(0, count), FIRST_LOTS]
            remote(part, part, send_plane, recv_plane.at[group], me ^ 1).wait_recv()
            members = pl.ds(pl.multiple_of((my_row ^ group) * 8, 8), 8)

            def send_to(target, lot):
                remote(
                    relay.at[members, lot], arrived.at[my_depth, members], send_depth, recv_depth, target
                ).start()

            both_cores(range(1), send_to)

        for group in GROUPS[:3]:
            pass_on(group)

        others = plane_tags.at[pl.ds(0, 2 * (PLANE - 1))]
        remote(others, others, send_tags, recv_tags, me ^ 1).wait_recv()
        column[...] = turned_tags(plane_tags)[: 4 * DEPTH]

        def send_column_to(target, lot):
            remote(
                column.at[two(lot)], depth_tags.at[two(my_depth)], send_column, recv_column, target
            ).start()

        def known(depth):
            return my_depth >= depth

        def unknown(depth):
            return my_depth < depth

        both_cores(range(1), send_column_to)
        both_cores(range(1, LATE), send_column_to, known)
        depth_tags[two(my_depth)] = column[two(my_depth * 2 + 1)]
        pass_on(GROUPS[3])
        def send_rest_to(target, lot):
            remote(relay.at[:, lot], arrived.at[my_depth], send_depth, recv_depth, target).start()

        for index, tier in enumerate(TIERS):
            part = relay.at[pl.ds(0, PLANE - 1), lots_of(tier)]
            remote(part, part, send_plane, recv_rest.at[index], me ^ 1).wait_recv()
            both_cores(range(tier[0], min(tier[1], LATE)), send_rest_to, known)
        await_column()
        both_cores(range(1, LATE), send_column_to, unknown)
        both_cores(range(LATE, DEPTH), send_column_to)
        both_cores(range(1, LATE), send_rest_to, unknown)
        both_cores(range(LATE, DEPTH), send_rest_to)
        arrived[my_depth] = relay[:, my_depth * 2 + 1]

        @pl.when(me != EARLIEST)
        def _():
            most = depth_tags.at[pl.ds(0, 2 * (DEPTH - 1))]
            remote(most, most, send_column, recv_column, me ^ 1).wait_recv()

        @pl.when(me == EARLIEST)
        def _():
            remote(direct_tags, direct_tags, send_direct, recv_direct, me ^ 1).wait_recv()
            turned = jnp.transpose(direct_tags[: 4 * PLANE])
            pair = turned[2 * EARLIEST : 2 * EARLIEST + 2]
            totals = jnp.broadcast_to(turned[4 * DEPTH : 4 * DEPTH + 1], (2, 128))
            lower = lax.broadcasted_iota(jnp.int32, (2, 128), 1) < 64
            depth_tags[2 * DIRECT[0] : 2 * DIRECT[0] + 2] = jnp.where(
                lower, pair, pltpu.roll(totals, 64, axis=1)
            )
            depth_tags[2 * DIRECT[1] : 2 * DIRECT[1] + 2] = jnp.where(
                lower, pltpu.roll(pair, 64, axis=1), totals
            )
            turned = turned_tags(direct_tags.at[pl.ds(4 * PLANE, 2 * PLANE)])
            depth_tags[2 * DIRECT[2] : 2 * DIRECT[2] + 2] = turned[2 * EARLIEST : 2 * EARLIEST + 2]
            most = depth_tags.at[pl.ds(0, 2 * (DEPTH - 1 - len(DIRECT)))]
            remote(most, most, send_column, recv_column, me ^ 1).wait_recv()

    half = lax.broadcasted_iota(jnp.int32, (1, 128), 1) < 64
    labels = lax.broadcasted_iota(jnp.int32, (BINS_DEV, 128), 0).astype(jnp.float32)
    totals = jnp.zeros((1, 128), jnp.float32)
    weighed = jnp.zeros((BINS_DEV, 128), jnp.float32)
    selectors = []
    for pair in range(DEPTH // 2):
        first = depth_tags[4 * pair : 4 * pair + 2]
        second = depth_tags[4 * pair + 2 : 4 * pair + 4]
        totals = totals + first[0:1] + second[0:1]
        turned = pltpu.roll(second, 64, axis=1)
        weight = jnp.where(half, first[0:1], turned[0:1])
        offset = jnp.where(half, first[1:2], turned[1:2])
        chosen = labels == offset
        weighed = weighed + jnp.where(chosen, weight, 0.0)
        selectors.append(jnp.where(chosen, 1.0, 0.0).astype(jnp.bfloat16))
    @pl.when(core == 0)
    def _():
        remote(everything, everything, send_depth, recv_depth, me ^ 1).wait_recv()

    @pl.when(core == 1)
    def _():
        most = arrived.at[pl.ds(0, DEPTH - 1)]
        remote(most, most, send_depth, recv_depth, me ^ 1).wait_recv()

    den = jnp.broadcast_to(jnp.sum(weighed, axis=1, keepdims=True), (BINS_DEV, 128)) + 1.0
    total = jnp.sum(jnp.where(half, 0.0, totals), axis=1, keepdims=True)
    rarity_ref[...] = jnp.log(total / (BINS_DEV * DEVICES)) - jnp.log(jnp.transpose(den)[0:1, :BINS_DEV])

    mean_ref[...] = jnp.dot(
        jnp.concatenate(selectors, axis=1), arrived.reshape(2 * DEVICES, 128)[...],
        preferred_element_type=jnp.float32,
    ) / den

    def sent(chips):
        part = packed.at[pl.ds(0, chips)]
        remote(part, part, send_plane, recv_plane.at[0], me ^ 1).wait_send()
        part = tags.at[pl.ds(0, 2 * chips)]
        remote(part, part, send_tags, recv_tags, me ^ 1).wait_send()

    @pl.when(core == 0)
    def _():
        sent(CHIPS)

    @pl.when(core == 1)
    def _():
        sent(CHIPS - 1)

    def relayed(targets):
        part = relay.at[pl.ds(0, 2 * targets)]
        remote(part, part, send_depth, recv_depth, me ^ 1).wait_send()
        part = column.at[pl.ds(0, 2 * targets)]
        remote(part, part, send_column, recv_column, me ^ 1).wait_send()

    pl.when((core == 1) & jnp.logical_not(bypassed))(functools.partial(relayed, 2 * DEPTH - 1))
    pl.when(bypassed)(functools.partial(relayed, 2 * DEPTH - 2))

    @pl.when(is_direct)
    def _():
        part = tags.at[two(0)]
        remote(part, part, send_direct, recv_direct, me ^ 1).wait_send()
        part = packed.at[0, EARLIEST]
        remote(part, part, send_rows, recv_depth, me ^ 1).wait_send()


def write_out(mean, rarity, mean_hbm, rarity_hbm, sems):
    copies = [
        pltpu.make_async_copy(mean, mean_hbm, sems.at[0]),
        pltpu.make_async_copy(rarity, rarity_hbm, sems.at[1]),
    ]
    for copy in copies:
        copy.start()
    for copy in copies:
        copy.wait()


def shards(goal_embed, goal_bins, goal_weights):
    width = goal_embed.shape[1]
    goals = goal_embed.shape[0]
    vmem = pl.BlockSpec(memory_space=pltpu.VMEM)
    hbm = pl.BlockSpec(memory_space=pltpu.HBM)
    dma = pltpu.SemaphoreType.DMA
    shapes = (
        jax.ShapeDtypeStruct((BINS_DEV, width), jnp.float32),
        jax.ShapeDtypeStruct((1, BINS_DEV), jnp.float32),
    )
    results = pl.pallas_call(
        exchange,
        out_shape=shapes,
        in_specs=[hbm] * 3,
        out_specs=(vmem, vmem),
        scratch_shapes=[
            pltpu.VMEM((goals, width), jnp.bfloat16),
            pltpu.VMEM((1, goals), jnp.int32),
            pltpu.VMEM((1, goals), jnp.float32),
            pltpu.VMEM((CHIPS, 2 * DEPTH, 2, width), jnp.bfloat16),
            pltpu.VMEM((PLANE, 2 * DEPTH, 2, width), jnp.bfloat16),
            pltpu.VMEM((DEPTH, PLANE, 2, width), jnp.bfloat16),
            pltpu.VMEM((2 * CHIPS, 128), jnp.float32),
            pltpu.VMEM((2 * PLANE, 128), jnp.float32),
            pltpu.VMEM((2 * len(DIRECT) * PLANE, 128), jnp.float32),
            pltpu.VMEM((4 * DEPTH, 128), jnp.float32),
            pltpu.VMEM((2 * DEPTH, 128), jnp.float32),
            dma((3,)), dma(()), dma((4,)), dma((len(TIERS),)), dma(()), dma(()), dma(()), dma(()), dma(()), dma(()),
            dma(()), dma(()), dma(()),
            pltpu.SemaphoreType.REGULAR, pltpu.SemaphoreType.REGULAR,
        ],
        compiler_params=pltpu.CompilerParams(collective_id=0, has_side_effects=True, vmem_limit_bytes=4 << 20),
        name="exchange",
    )(*[
        pltpu.with_memory_space_constraint(array, pltpu.HBM)
        for array in (goal_embed, goal_bins.reshape(1, goals), goal_weights.reshape(1, goals))
    ])
    mean, rarity = pl.pallas_call(
        write_out,
        out_shape=shapes,
        in_specs=[vmem, vmem],
        out_specs=(hbm, hbm),
        scratch_shapes=[dma((2,))],
        compiler_params=pltpu.CompilerParams(vmem_limit_bytes=1 << 20),
        name="write_out",
    )(*results)
    return mean, rarity[0]


def solution(mesh):
    flat = Mesh(mesh.devices.reshape(-1), (AXIS,))
    return jax.shard_map(
        shards, mesh=flat, in_specs=(P(AXIS, None), P(AXIS), P(AXIS)),
        out_specs=(P(AXIS, None), P(AXIS)), check_vma=False,
    )
```

```python
import functools

import jax
import jax.numpy as jnp
from jax import lax
from jax.experimental import pallas as pl
from jax.experimental.pallas import tpu as pltpu
from jax.sharding import Mesh
from jax.sharding import PartitionSpec as P

BINS_DEV = 64
AXIS = "device"
LOGICAL = pl.DeviceIdType.LOGICAL
DEVICES = 256
CHIPS = 16
PLANE = 32
DEPTH = 8
HOPS = (0, 1, 2, 1)
STEPS = sorted(range(1, CHIPS), key=lambda step: -(HOPS[step >> 2] + HOPS[step & 3]))
GROUPS = (0, 3, 1, 2)
FIRST_LOTS = pl.ds(0, 2)
TIERS = ((1, 3), (3, 8))


def lots_of(tier):
    return pl.ds(2 * tier[0], 2 * (tier[1] - tier[0]))


LATE = 4
EARLIEST = 1
DIRECT = (4, 5, 6)
BYPASSED = (129, 137, 193)


def depth_of(flat):
    return ((flat >> 6) << 1) | ((flat >> 3) & 1)


def chip_of(flat):
    return (((flat >> 4) & 3) << 2) | ((flat >> 1) & 3)


def flat_of_chip(chip):
    return ((chip >> 2) << 4) | ((chip & 3) << 1)


def flat_of_depth(depth):
    return ((depth >> 1) << 6) | ((depth & 1) << 3)


def remote(src, dst, send, recv, target):
    return pltpu.make_async_remote_copy(
        src_ref=src, dst_ref=dst, send_sem=send, recv_sem=recv, device_id=target, device_id_type=LOGICAL
    )


def two(index):
    return pl.ds(pl.multiple_of(2 * index, 2), 2)


def turned_tags(tags_ref):
    turned = jnp.transpose(tags_ref[...])
    wide = jnp.concatenate([turned[: 4 * DEPTH], turned[: 4 * DEPTH]], axis=1)
    total = jnp.concatenate([turned[4 * DEPTH : 4 * DEPTH + 1]] * 2, axis=1)
    lower = lax.broadcasted_iota(jnp.int32, (4 * DEPTH, 128), 1) < 2 * PLANE
    return jnp.where(lower, wide, total)


def exchange(
    embed_hbm, bins_hbm, weights_hbm, mean_ref, rarity_ref,
    embed, bins, weights, packed, relay, arrived, tags, plane_tags, direct_tags, column, depth_tags,
    in_sems, send_plane, recv_plane, recv_rest, send_depth, recv_depth,
    send_tags, recv_tags, send_column, recv_column, send_direct, recv_direct, send_rows, above_ready, below_ready,
):
    me = lax.axis_index(AXIS)
    core = me & 1
    my_depth = depth_of(me)
    my_chip = chip_of(me)
    my_place = my_chip * 2 + core
    my_row = my_chip >> 2
    bottom = flat_of_chip(my_chip)
    loads = [
        pltpu.make_async_copy(bins_hbm, bins, in_sems.at[0]),
        pltpu.make_async_copy(weights_hbm, weights, in_sems.at[1]),
        pltpu.make_async_copy(embed_hbm, embed, in_sems.at[2]),
    ]
    for load in loads:
        load.start()
    barrier = pltpu.get_barrier_semaphore()

    def greet(target):
        pl.semaphore_signal(barrier, inc=1, device_id=target, device_id_type=LOGICAL)

    def relays(first, last, act):
        def visit(depth, carry):
            act(bottom | flat_of_depth(depth) | 1)
            return carry

        lax.fori_loop(first, last, visit, 0)

    greet(me ^ 1)

    @pl.when(core == 1)
    def _():
        for step in STEPS:
            greet(me ^ flat_of_chip(step))
            greet(me ^ flat_of_chip(step) ^ 1)

    @pl.when((core == 1) | (my_depth < LATE))
    def _():
        relays(my_depth + 1, DEPTH, greet)

    @pl.when(me == EARLIEST)
    def _():
        for place in range(PLANE - 1, -1, -1):
            for depth in DIRECT:
                target = flat_of_depth(depth) | flat_of_chip(place >> 1) | (place & 1)
                if target not in BYPASSED:
                    greet(target)

    is_direct = (my_depth >= DIRECT[0]) & (my_depth <= DIRECT[-1])
    bypassed = is_direct & (my_chip == 0) & (core == 1)
    one_more = is_direct.astype(jnp.int32)

    for load in loads:
        load.wait()

    lanes = lax.broadcasted_iota(jnp.int32, (128, 128), 1)
    rows = lax.broadcasted_iota(jnp.int32, (128, 128), 0)
    bin_row = jnp.broadcast_to(bins[...], (128, 128))
    weight_row = jnp.broadcast_to(weights[...], (128, 128))
    bin_col = jnp.transpose(bin_row.astype(jnp.float32)).astype(jnp.int32)
    weight_col = jnp.transpose(weight_row)
    owner_row = bin_row >> 6
    owner_col = bin_col >> 6
    earlier = jnp.where((owner_row == owner_col) & (rows < lanes), 1.0, 0.0)
    slot_of = jnp.sum(earlier, axis=0, keepdims=True).astype(jnp.int32)
    owner = bins[...] >> 6
    row_id = ((chip_of(owner) * DEPTH + depth_of(owner)) * 2 + (owner & 1)) * 2 + slot_of
    tag_id = chip_of(owner) * 2 + slot_of

    lane_of = (depth_of(owner_col) * 2 + (owner_col & 1)) * 2
    offset_col = (bin_col & (BINS_DEV - 1)).astype(jnp.float32)
    values = jnp.where(lanes == lane_of, weight_col, 0.0) + jnp.where(lanes == lane_of + 1, offset_col, 0.0)
    tag_lanes = lax.broadcasted_iota(jnp.int32, (2 * CHIPS, 128), 1)
    tag_rows = lax.broadcasted_iota(jnp.int32, (2 * CHIPS, 128), 0)
    tag_pick = (tag_rows == tag_id).astype(jnp.float32)
    local_total = jnp.sum(weights[...])
    tags[...] = jnp.dot(
        tag_pick, values, precision=lax.Precision.HIGHEST, preferred_element_type=jnp.float32
    ) + jnp.where((tag_lanes == 4 * DEPTH) & (tag_rows % 2 == 0), local_total, 0.0)

    scaled = (weight_col * embed[...].astype(jnp.float32)).astype(jnp.bfloat16)
    pick = (lax.broadcasted_iota(jnp.int32, (2 * DEVICES, 128), 0) == row_id).astype(jnp.float32)
    packed.reshape(2 * DEVICES, 128)[...] = jnp.dot(
        pick.astype(jnp.bfloat16), scaled, preferred_element_type=jnp.float32
    ).astype(jnp.bfloat16)

    def hand_tags(chip, target):
        remote(tags.at[two(chip)], plane_tags.at[two(my_place)], send_tags, recv_tags, target).start()

    def hand_first(chip, target, group):
        remote(
            packed.at[chip, FIRST_LOTS], relay.at[my_place, FIRST_LOTS],
            send_plane, recv_plane.at[group], target,
        ).start()

    def hand_tier(index, chip, target):
        lots = lots_of(TIERS[index])
        remote(
            packed.at[chip, lots], relay.at[my_place, lots], send_plane, recv_rest.at[index], target
        ).start()

    def hand_direct():
        row = (my_depth - DIRECT[0]) * PLANE + my_place
        remote(tags.at[two(0)], direct_tags.at[two(row)], send_direct, recv_direct, EARLIEST).start()
        remote(
            packed.at[0, EARLIEST], arrived.at[my_depth, my_place], send_rows, recv_depth, EARLIEST
        ).start()

    def hand_all():
        pl.when(is_direct)(hand_direct)
        for step in STEPS:
            hand_tags(my_chip ^ step, (me ^ flat_of_chip(step)) | 1)
            hand_first(my_chip ^ step, (me ^ flat_of_chip(step)) | 1, step >> 2)

    everything = arrived.at[pl.ds(0, DEPTH)]
    all_tags = pl.ds(0, 2 * DEPTH)

    @pl.when(core == 0)
    def _():
        pl.semaphore_wait(barrier, CHIPS + one_more)
        hand_all()
        hand_tags(my_chip, me ^ 1)
        hand_first(my_chip, me ^ 1, 0)
        for index in range(len(TIERS)):
            for step in STEPS:
                hand_tier(index, my_chip ^ step, (me ^ flat_of_chip(step)) | 1)
            hand_tier(index, my_chip, me ^ 1)
        remote(depth_tags.at[all_tags], depth_tags.at[all_tags], send_column, recv_column, me ^ 1).wait_recv()

    @pl.when(core == 1)
    def _():
        greeted = my_depth + jnp.minimum(my_depth, LATE) + jnp.where(bypassed, 0, one_more)
        pl.semaphore_wait(barrier, CHIPS + greeted)
        hand_all()

        def answer(target):
            pl.semaphore_signal(above_ready, inc=1, device_id=target, device_id_type=LOGICAL)

        relays(0, my_depth, answer)
        for index in range(len(TIERS)):
            for step in STEPS:
                hand_tier(index, my_chip ^ step, (me ^ flat_of_chip(step)) | 1)
        relay[my_place] = packed[my_chip]
        plane_tags[two(my_place)] = tags[two(my_chip)]

        @pl.when((my_depth >= LATE) & (my_depth < DEPTH - 1))
        def _():
            pl.semaphore_wait(above_ready, DEPTH - 1 - my_depth)

            def answer_late(target):
                pl.semaphore_signal(below_ready, inc=1, device_id=target, device_id_type=LOGICAL)

            relays(my_depth + 1, DEPTH, answer_late)

        def await_column():
            @pl.when(my_depth > LATE)
            def _():
                pl.semaphore_wait(below_ready, my_depth - LATE)

            @pl.when(my_depth < LATE)
            def _():
                pl.semaphore_wait(above_ready, DEPTH - 1 - my_depth)

        def both_cores(depths, send_to, only=None):
            for depth in depths:
                column_at = bottom | flat_of_depth(depth)
                wanted = my_depth != depth
                chosen = True if only is None else only(depth)
                if only is not None:
                    wanted = wanted & chosen
                if depth == 0:
                    wanted = wanted & jnp.logical_not(bypassed)
                pl.when(wanted)(functools.partial(send_to, column_at | 1, 2 * depth + 1))
                if only is None:
                    send_to(column_at, 2 * depth)
                else:
                    pl.when(chosen)(functools.partial(send_to, column_at, 2 * depth))

        def pass_on(group):
            count = 8 if group else 7
            part = relay.at[pl.ds(0, count), FIRST_LOTS]
            remote(part, part, send_plane, recv_plane.at[group], me ^ 1).wait_recv()
            members = pl.ds(pl.multiple_of((my_row ^ group) * 8, 8), 8)

            def send_to(target, lot):
                remote(
                    relay.at[members, lot], arrived.at[my_depth, members], send_depth, recv_depth, target
                ).start()

            both_cores(range(1), send_to)

        for group in GROUPS[:3]:
            pass_on(group)

        others = plane_tags.at[pl.ds(0, 2 * (PLANE - 1))]
        remote(others, others, send_tags, recv_tags, me ^ 1).wait_recv()
        column[...] = turned_tags(plane_tags)[: 4 * DEPTH]

        def send_column_to(target, lot):
            remote(
                column.at[two(lot)], depth_tags.at[two(my_depth)], send_column, recv_column, target
            ).start()

        def known(depth):
            return my_depth >= depth

        def unknown(depth):
            return my_depth < depth

        both_cores(range(1), send_column_to)
        depth_tags[two(my_depth)] = column[two(my_depth * 2 + 1)]
        pass_on(GROUPS[3])
        both_cores(range(1, LATE), send_column_to, known)
        def send_rest_to(target, lot):
            remote(relay.at[:, lot], arrived.at[my_depth], send_depth, recv_depth, target).start()

        for index, tier in enumerate(TIERS):
            part = relay.at[pl.ds(0, PLANE - 1), lots_of(tier)]
            remote(part, part, send_plane, recv_rest.at[index], me ^ 1).wait_recv()
            both_cores(range(tier[0], min(tier[1], LATE)), send_rest_to, known)
        await_column()
        both_cores(range(1, LATE), send_column_to, unknown)
        both_cores(range(LATE, DEPTH), send_column_to)
        both_cores(range(1, LATE), send_rest_to, unknown)
        both_cores(range(LATE, DEPTH), send_rest_to)
        arrived[my_depth] = relay[:, my_depth * 2 + 1]

        @pl.when(me != EARLIEST)
        def _():
            most = depth_tags.at[pl.ds(0, 2 * (DEPTH - 1))]
            remote(most, most, send_column, recv_column, me ^ 1).wait_recv()

        @pl.when(me == EARLIEST)
        def _():
            remote(direct_tags, direct_tags, send_direct, recv_direct, me ^ 1).wait_recv()
            turned = jnp.transpose(direct_tags[: 4 * PLANE])
            pair = turned[2 * EARLIEST : 2 * EARLIEST + 2]
            totals = jnp.broadcast_to(turned[4 * DEPTH : 4 * DEPTH + 1], (2, 128))
            lower = lax.broadcasted_iota(jnp.int32, (2, 128), 1) < 64
            depth_tags[2 * DIRECT[0] : 2 * DIRECT[0] + 2] = jnp.where(
                lower, pair, pltpu.roll(totals, 64, axis=1)
            )
            depth_tags[2 * DIRECT[1] : 2 * DIRECT[1] + 2] = jnp.where(
                lower, pltpu.roll(pair, 64, axis=1), totals
            )
            turned = turned_tags(direct_tags.at[pl.ds(4 * PLANE, 2 * PLANE)])
            depth_tags[2 * DIRECT[2] : 2 * DIRECT[2] + 2] = turned[2 * EARLIEST : 2 * EARLIEST + 2]
            most = depth_tags.at[pl.ds(0, 2 * (DEPTH - 1 - len(DIRECT)))]
            remote(most, most, send_column, recv_column, me ^ 1).wait_recv()

    half = lax.broadcasted_iota(jnp.int32, (1, 128), 1) < 64
    labels = lax.broadcasted_iota(jnp.int32, (BINS_DEV, 128), 0).astype(jnp.float32)
    totals = jnp.zeros((1, 128), jnp.float32)
    weighed = jnp.zeros((BINS_DEV, 128), jnp.float32)
    selectors = []
    for pair in range(DEPTH // 2):
        first = depth_tags[4 * pair : 4 * pair + 2]
        second = depth_tags[4 * pair + 2 : 4 * pair + 4]
        totals = totals + first[0:1] + second[0:1]
        turned = pltpu.roll(second, 64, axis=1)
        weight = jnp.where(half, first[0:1], turned[0:1])
        offset = jnp.where(half, first[1:2], turned[1:2])
        chosen = labels == offset
        weighed = weighed + jnp.where(chosen, weight, 0.0)
        selectors.append(jnp.where(chosen, 1.0, 0.0).astype(jnp.bfloat16))
    @pl.when(core == 0)
    def _():
        remote(everything, everything, send_depth, recv_depth, me ^ 1).wait_recv()

    @pl.when(core == 1)
    def _():
        most = arrived.at[pl.ds(0, DEPTH - 1)]
        remote(most, most, send_depth, recv_depth, me ^ 1).wait_recv()

    den = jnp.broadcast_to(jnp.sum(weighed, axis=1, keepdims=True), (BINS_DEV, 128)) + 1.0
    total = jnp.sum(jnp.where(half, 0.0, totals), axis=1, keepdims=True)
    rarity_ref[...] = jnp.log(total / (BINS_DEV * DEVICES)) - jnp.log(jnp.transpose(den)[0:1, :BINS_DEV])

    mean_ref[...] = jnp.dot(
        jnp.concatenate(selectors, axis=1), arrived.reshape(2 * DEVICES, 128)[...],
        preferred_element_type=jnp.float32,
    ) / den

    def sent(chips):
        part = packed.at[pl.ds(0, chips)]
        remote(part, part, send_plane, recv_plane.at[0], me ^ 1).wait_send()
        part = tags.at[pl.ds(0, 2 * chips)]
        remote(part, part, send_tags, recv_tags, me ^ 1).wait_send()

    @pl.when(core == 0)
    def _():
        sent(CHIPS)

    @pl.when(core == 1)
    def _():
        sent(CHIPS - 1)

    def relayed(targets):
        part = relay.at[pl.ds(0, 2 * targets)]
        remote(part, part, send_depth, recv_depth, me ^ 1).wait_send()
        part = column.at[pl.ds(0, 2 * targets)]
        remote(part, part, send_column, recv_column, me ^ 1).wait_send()

    pl.when((core == 1) & jnp.logical_not(bypassed))(functools.partial(relayed, 2 * DEPTH - 1))
    pl.when(bypassed)(functools.partial(relayed, 2 * DEPTH - 2))

    @pl.when(is_direct)
    def _():
        part = tags.at[two(0)]
        remote(part, part, send_direct, recv_direct, me ^ 1).wait_send()
        part = packed.at[0, EARLIEST]
        remote(part, part, send_rows, recv_depth, me ^ 1).wait_send()


def write_out(mean, rarity, mean_hbm, rarity_hbm, sems):
    copies = [
        pltpu.make_async_copy(mean, mean_hbm, sems.at[0]),
        pltpu.make_async_copy(rarity, rarity_hbm, sems.at[1]),
    ]
    for copy in copies:
        copy.start()
    for copy in copies:
        copy.wait()


def shards(goal_embed, goal_bins, goal_weights):
    width = goal_embed.shape[1]
    goals = goal_embed.shape[0]
    vmem = pl.BlockSpec(memory_space=pltpu.VMEM)
    hbm = pl.BlockSpec(memory_space=pltpu.HBM)
    dma = pltpu.SemaphoreType.DMA
    shapes = (
        jax.ShapeDtypeStruct((BINS_DEV, width), jnp.float32),
        jax.ShapeDtypeStruct((1, BINS_DEV), jnp.float32),
    )
    results = pl.pallas_call(
        exchange,
        out_shape=shapes,
        in_specs=[hbm] * 3,
        out_specs=(vmem, vmem),
        scratch_shapes=[
            pltpu.VMEM((goals, width), jnp.bfloat16),
            pltpu.VMEM((1, goals), jnp.int32),
            pltpu.VMEM((1, goals), jnp.float32),
            pltpu.VMEM((CHIPS, 2 * DEPTH, 2, width), jnp.bfloat16),
            pltpu.VMEM((PLANE, 2 * DEPTH, 2, width), jnp.bfloat16),
            pltpu.VMEM((DEPTH, PLANE, 2, width), jnp.bfloat16),
            pltpu.VMEM((2 * CHIPS, 128), jnp.float32),
            pltpu.VMEM((2 * PLANE, 128), jnp.float32),
            pltpu.VMEM((2 * len(DIRECT) * PLANE, 128), jnp.float32),
            pltpu.VMEM((4 * DEPTH, 128), jnp.float32),
            pltpu.VMEM((2 * DEPTH, 128), jnp.float32),
            dma((3,)), dma(()), dma((4,)), dma((len(TIERS),)), dma(()), dma(()), dma(()), dma(()), dma(()), dma(()),
            dma(()), dma(()), dma(()),
            pltpu.SemaphoreType.REGULAR, pltpu.SemaphoreType.REGULAR,
        ],
        compiler_params=pltpu.CompilerParams(collective_id=0, has_side_effects=True, vmem_limit_bytes=4 << 20),
        name="exchange",
    )(*[
        pltpu.with_memory_space_constraint(array, pltpu.HBM)
        for array in (goal_embed, goal_bins.reshape(1, goals), goal_weights.reshape(1, goals))
    ])
    mean, rarity = pl.pallas_call(
        write_out,
        out_shape=shapes,
        in_specs=[vmem, vmem],
        out_specs=(hbm, hbm),
        scratch_shapes=[dma((2,))],
        compiler_params=pltpu.CompilerParams(vmem_limit_bytes=1 << 20),
        name="write_out",
    )(*results)
    return mean, rarity[0]


def solution(mesh):
    flat = Mesh(mesh.devices.reshape(-1), (AXIS,))
    return jax.shard_map(
        shards, mesh=flat, in_specs=(P(AXIS, None), P(AXIS), P(AXIS)),
        out_specs=(P(AXIS, None), P(AXIS)), check_vma=False,
    )
```

```python
import functools

import jax
import jax.numpy as jnp
from jax import lax
from jax.experimental import pallas as pl
from jax.experimental.pallas import tpu as pltpu
from jax.sharding import Mesh
from jax.sharding import PartitionSpec as P

BINS_DEV = 64
AXIS = "device"
LOGICAL = pl.DeviceIdType.LOGICAL
DEVICES = 256
CHIPS = 16
PLANE = 32
DEPTH = 8
HOPS = (0, 1, 2, 1)
STEPS = sorted(range(1, CHIPS), key=lambda step: -(HOPS[step >> 2] + HOPS[step & 3]))
GROUPS = (0, 3, 1, 2)
FIRST_LOTS = pl.ds(0, 2)
TIERS = ((1, 3), (3, 8))


def lots_of(tier):
    return pl.ds(2 * tier[0], 2 * (tier[1] - tier[0]))


LATE = 4
EARLIEST = 1
DIRECT = (4, 5, 6)
BYPASSED = (129, 137, 193)


def depth_of(flat):
    return ((flat >> 6) << 1) | ((flat >> 3) & 1)


def chip_of(flat):
    return (((flat >> 4) & 3) << 2) | ((flat >> 1) & 3)


def flat_of_chip(chip):
    return ((chip >> 2) << 4) | ((chip & 3) << 1)


def flat_of_depth(depth):
    return ((depth >> 1) << 6) | ((depth & 1) << 3)


def remote(src, dst, send, recv, target):
    return pltpu.make_async_remote_copy(
        src_ref=src, dst_ref=dst, send_sem=send, recv_sem=recv, device_id=target, device_id_type=LOGICAL
    )


def two(index):
    return pl.ds(pl.multiple_of(2 * index, 2), 2)


def turned_tags(tags_ref):
    plane = tags_ref[...]
    totals = jnp.broadcast_to(plane[:, 4 * DEPTH : 4 * DEPTH + 1], (2 * PLANE, 128))
    return jnp.transpose(jnp.concatenate([plane, totals], axis=0))


def exchange(
    embed_hbm, bins_hbm, weights_hbm, mean_ref, rarity_ref,
    embed, bins, weights, packed, relay, arrived, tags, plane_tags, direct_tags, column, depth_tags,
    in_sems, send_plane, recv_plane, recv_rest, send_depth, recv_depth,
    send_tags, recv_tags, send_column, recv_column, send_direct, recv_direct, send_rows, above_ready, below_ready,
):
    me = lax.axis_index(AXIS)
    core = me & 1
    my_depth = depth_of(me)
    my_chip = chip_of(me)
    my_place = my_chip * 2 + core
    my_row = my_chip >> 2
    bottom = flat_of_chip(my_chip)
    loads = [
        pltpu.make_async_copy(bins_hbm, bins, in_sems.at[0]),
        pltpu.make_async_copy(weights_hbm, weights, in_sems.at[1]),
        pltpu.make_async_copy(embed_hbm, embed, in_sems.at[2]),
    ]
    for load in loads:
        load.start()
    barrier = pltpu.get_barrier_semaphore()

    def greet(target):
        pl.semaphore_signal(barrier, inc=1, device_id=target, device_id_type=LOGICAL)

    def relays(first, last, act):
        def visit(depth, carry):
            act(bottom | flat_of_depth(depth) | 1)
            return carry

        lax.fori_loop(first, last, visit, 0)

    greet(me ^ 1)

    @pl.when(core == 1)
    def _():
        for step in STEPS:
            greet(me ^ flat_of_chip(step))
            greet(me ^ flat_of_chip(step) ^ 1)

    @pl.when((core == 1) | (my_depth < LATE))
    def _():
        relays(my_depth + 1, DEPTH, greet)

    @pl.when(me == EARLIEST)
    def _():
        for place in range(PLANE - 1, -1, -1):
            for depth in DIRECT:
                target = flat_of_depth(depth) | flat_of_chip(place >> 1) | (place & 1)
                if target not in BYPASSED:
                    greet(target)

    is_direct = (my_depth >= DIRECT[0]) & (my_depth <= DIRECT[-1])
    bypassed = is_direct & (my_chip == 0) & (core == 1)
    one_more = is_direct.astype(jnp.int32)

    for load in loads:
        load.wait()

    lanes = lax.broadcasted_iota(jnp.int32, (128, 128), 1)
    rows = lax.broadcasted_iota(jnp.int32, (128, 128), 0)
    bin_row = jnp.broadcast_to(bins[...], (128, 128))
    weight_row = jnp.broadcast_to(weights[...], (128, 128))
    bin_col = jnp.transpose(bin_row.astype(jnp.float32)).astype(jnp.int32)
    weight_col = jnp.transpose(weight_row)
    owner_row = bin_row >> 6
    owner_col = bin_col >> 6
    earlier = jnp.where((owner_row == owner_col) & (rows < lanes), 1.0, 0.0)
    slot_of = jnp.sum(earlier, axis=0, keepdims=True).astype(jnp.int32)
    owner = bins[...] >> 6
    row_id = ((chip_of(owner) * DEPTH + depth_of(owner)) * 2 + (owner & 1)) * 2 + slot_of
    tag_id = chip_of(owner) * 2 + slot_of

    lane_of = (depth_of(owner_col) * 2 + (owner_col & 1)) * 2
    offset_col = (bin_col & (BINS_DEV - 1)).astype(jnp.float32)
    values = jnp.where(lanes == lane_of, weight_col, 0.0) + jnp.where(lanes == lane_of + 1, offset_col, 0.0)
    tag_lanes = lax.broadcasted_iota(jnp.int32, (2 * CHIPS, 128), 1)
    tag_rows = lax.broadcasted_iota(jnp.int32, (2 * CHIPS, 128), 0)
    tag_pick = (tag_rows == tag_id).astype(jnp.float32)
    local_total = jnp.sum(weights[...])
    tags[...] = jnp.dot(
        tag_pick, values, precision=lax.Precision.HIGHEST, preferred_element_type=jnp.float32
    ) + jnp.where((tag_lanes == 4 * DEPTH) & (tag_rows % 2 == 0), local_total, 0.0)

    scaled = (weight_col * embed[...].astype(jnp.float32)).astype(jnp.bfloat16)
    pick = (lax.broadcasted_iota(jnp.int32, (2 * DEVICES, 128), 0) == row_id).astype(jnp.float32)
    packed.reshape(2 * DEVICES, 128)[...] = jnp.dot(
        pick.astype(jnp.bfloat16), scaled, preferred_element_type=jnp.float32
    ).astype(jnp.bfloat16)

    def hand_tags(chip, target):
        remote(tags.at[two(chip)], plane_tags.at[two(my_place)], send_tags, recv_tags, target).start()

    def hand_first(chip, target, group):
        remote(
            packed.at[chip, FIRST_LOTS], relay.at[my_place, FIRST_LOTS],
            send_plane, recv_plane.at[group], target,
        ).start()

    def hand_tier(index, chip, target):
        lots = lots_of(TIERS[index])
        remote(
            packed.at[chip, lots], relay.at[my_place, lots], send_plane, recv_rest.at[index], target
        ).start()

    def hand_direct():
        row = (my_depth - DIRECT[0]) * PLANE + my_place
        remote(tags.at[two(0)], direct_tags.at[two(row)], send_direct, recv_direct, EARLIEST).start()
        remote(
            packed.at[0, EARLIEST], arrived.at[my_depth, my_place], send_rows, recv_depth, EARLIEST
        ).start()

    def hand_all():
        pl.when(is_direct)(hand_direct)
        for step in STEPS:
            hand_tags(my_chip ^ step, (me ^ flat_of_chip(step)) | 1)
            hand_first(my_chip ^ step, (me ^ flat_of_chip(step)) | 1, step >> 2)

    everything = arrived.at[pl.ds(0, DEPTH)]
    all_tags = pl.ds(0, 2 * DEPTH)

    @pl.when(core == 0)
    def _():
        pl.semaphore_wait(barrier, CHIPS + one_more)
        hand_all()
        hand_tags(my_chip, me ^ 1)
        hand_first(my_chip, me ^ 1, 0)
        for index in range(len(TIERS)):
            for step in STEPS:
                hand_tier(index, my_chip ^ step, (me ^ flat_of_chip(step)) | 1)
            hand_tier(index, my_chip, me ^ 1)
        remote(depth_tags.at[all_tags], depth_tags.at[all_tags], send_column, recv_column, me ^ 1).wait_recv()

    @pl.when(core == 1)
    def _():
        greeted = my_depth + jnp.minimum(my_depth, LATE) + jnp.where(bypassed, 0, one_more)
        pl.semaphore_wait(barrier, CHIPS + greeted)
        hand_all()

        def answer(target):
            pl.semaphore_signal(above_ready, inc=1, device_id=target, device_id_type=LOGICAL)

        relays(0, my_depth, answer)
        for index in range(len(TIERS)):
            for step in STEPS:
                hand_tier(index, my_chip ^ step, (me ^ flat_of_chip(step)) | 1)
        relay[my_place] = packed[my_chip]
        plane_tags[two(my_place)] = tags[two(my_chip)]

        @pl.when((my_depth >= LATE) & (my_depth < DEPTH - 1))
        def _():
            pl.semaphore_wait(above_ready, DEPTH - 1 - my_depth)

            def answer_late(target):
                pl.semaphore_signal(below_ready, inc=1, device_id=target, device_id_type=LOGICAL)

            relays(my_depth + 1, DEPTH, answer_late)

        def await_column():
            @pl.when(my_depth > LATE)
            def _():
                pl.semaphore_wait(below_ready, my_depth - LATE)

            @pl.when(my_depth < LATE)
            def _():
                pl.semaphore_wait(above_ready, DEPTH - 1 - my_depth)

        def both_cores(depths, send_to, only=None):
            for depth in depths:
                column_at = bottom | flat_of_depth(depth)
                wanted = my_depth != depth
                chosen = None if only is None else only(depth)
                if chosen is not None:
                    wanted = wanted & chosen
                if depth == 0:
                    wanted = wanted & jnp.logical_not(bypassed)

                def serve(core, depth=depth, column_at=column_at, wanted=wanted, chosen=chosen):
                    act = functools.partial(send_to, column_at | core, 2 * depth + core)
                    condition = wanted if core else chosen
                    if condition is None:
                        act()
                    else:
                        pl.when(condition)(act)

                for core in (1, 0) if depth == 0 else (0, 1):
                    serve(core)

        def pass_on(group):
            count = 8 if group else 7
            part = relay.at[pl.ds(0, count), FIRST_LOTS]
            remote(part, part, send_plane, recv_plane.at[group], me ^ 1).wait_recv()
            members = pl.ds(pl.multiple_of((my_row ^ group) * 8, 8), 8)

            def send_to(target, lot):
                remote(
                    relay.at[members, lot], arrived.at[my_depth, members], send_depth, recv_depth, target
                ).start()

            both_cores(range(1), send_to)

        for group in GROUPS[:3]:
            pass_on(group)

        others = plane_tags.at[pl.ds(0, 2 * (PLANE - 1))]
        remote(others, others, send_tags, recv_tags, me ^ 1).wait_recv()
        column[...] = turned_tags(plane_tags)[: 4 * DEPTH]

        def send_column_to(target, lot):
            remote(
                column.at[two(lot)], depth_tags.at[two(my_depth)], send_column, recv_column, target
            ).start()

        def known(depth):
            return my_depth >= depth

        def unknown(depth):
            return my_depth < depth

        both_cores(range(1), send_column_to)
        both_cores(range(1, LATE), send_column_to, known)
        depth_tags[two(my_depth)] = column[two(my_depth * 2 + 1)]
        pass_on(GROUPS[3])
        def send_rest_to(target, lot):
            remote(relay.at[:, lot], arrived.at[my_depth], send_depth, recv_depth, target).start()

        for index, tier in enumerate(TIERS):
            part = relay.at[pl.ds(0, PLANE - 1), lots_of(tier)]
            remote(part, part, send_plane, recv_rest.at[index], me ^ 1).wait_recv()
            both_cores(range(tier[0], min(tier[1], LATE)), send_rest_to, known)
        await_column()
        both_cores(range(1, LATE), send_column_to, unknown)
        both_cores(range(LATE, DEPTH), send_column_to)
        both_cores(range(1, LATE), send_rest_to, unknown)
        both_cores(range(LATE, DEPTH), send_rest_to)
        arrived[my_depth] = relay[:, my_depth * 2 + 1]

        @pl.when(me != EARLIEST)
        def _():
            most = depth_tags.at[pl.ds(0, 2 * (DEPTH - 1))]
            remote(most, most, send_column, recv_column, me ^ 1).wait_recv()

        @pl.when(me == EARLIEST)
        def _():
            remote(direct_tags, direct_tags, send_direct, recv_direct, me ^ 1).wait_recv()
            turned = jnp.transpose(direct_tags[: 4 * PLANE])
            pair = turned[2 * EARLIEST : 2 * EARLIEST + 2]
            totals = jnp.broadcast_to(turned[4 * DEPTH : 4 * DEPTH + 1], (2, 128))
            lower = lax.broadcasted_iota(jnp.int32, (2, 128), 1) < 64
            depth_tags[2 * DIRECT[0] : 2 * DIRECT[0] + 2] = jnp.where(
                lower, pair, pltpu.roll(totals, 64, axis=1)
            )
            depth_tags[2 * DIRECT[1] : 2 * DIRECT[1] + 2] = jnp.where(
                lower, pltpu.roll(pair, 64, axis=1), totals
            )
            turned = turned_tags(direct_tags.at[pl.ds(4 * PLANE, 2 * PLANE)])
            depth_tags[2 * DIRECT[2] : 2 * DIRECT[2] + 2] = turned[2 * EARLIEST : 2 * EARLIEST + 2]
            most = depth_tags.at[pl.ds(0, 2 * (DEPTH - 1 - len(DIRECT)))]
            remote(most, most, send_column, recv_column, me ^ 1).wait_recv()

    half = lax.broadcasted_iota(jnp.int32, (1, 128), 1) < 64
    labels = lax.broadcasted_iota(jnp.int32, (BINS_DEV, 128), 0).astype(jnp.float32)
    totals = jnp.zeros((1, 128), jnp.float32)
    weighed = jnp.zeros((BINS_DEV, 128), jnp.float32)
    selectors = []
    for pair in range(DEPTH // 2):
        first = depth_tags[4 * pair : 4 * pair + 2]
        second = depth_tags[4 * pair + 2 : 4 * pair + 4]
        totals = totals + first[0:1] + second[0:1]
        turned = pltpu.roll(second, 64, axis=1)
        weight = jnp.where(half, first[0:1], turned[0:1])
        offset = jnp.where(half, first[1:2], turned[1:2])
        chosen = labels == offset
        weighed = weighed + jnp.where(chosen, weight, 0.0)
        selectors.append(jnp.where(chosen, 1.0, 0.0).astype(jnp.bfloat16))
    @pl.when(core == 0)
    def _():
        remote(everything, everything, send_depth, recv_depth, me ^ 1).wait_recv()

    @pl.when(core == 1)
    def _():
        most = arrived.at[pl.ds(0, DEPTH - 1)]
        remote(most, most, send_depth, recv_depth, me ^ 1).wait_recv()

    den = jnp.broadcast_to(jnp.sum(weighed, axis=1, keepdims=True), (BINS_DEV, 128)) + 1.0
    total = jnp.sum(jnp.where(half, 0.0, totals), axis=1, keepdims=True)
    rarity_ref[...] = jnp.log(total / (BINS_DEV * DEVICES)) - jnp.log(jnp.transpose(den)[0:1, :BINS_DEV])

    mean_ref[...] = jnp.dot(
        jnp.concatenate(selectors, axis=1), arrived.reshape(2 * DEVICES, 128)[...],
        preferred_element_type=jnp.float32,
    ) / den

    def sent(chips):
        part = packed.at[pl.ds(0, chips)]
        remote(part, part, send_plane, recv_plane.at[0], me ^ 1).wait_send()
        part = tags.at[pl.ds(0, 2 * chips)]
        remote(part, part, send_tags, recv_tags, me ^ 1).wait_send()

    @pl.when(core == 0)
    def _():
        sent(CHIPS)

    @pl.when(core == 1)
    def _():
        sent(CHIPS - 1)

    def relayed(targets):
        part = relay.at[pl.ds(0, 2 * targets)]
        remote(part, part, send_depth, recv_depth, me ^ 1).wait_send()
        part = column.at[pl.ds(0, 2 * targets)]
        remote(part, part, send_column, recv_column, me ^ 1).wait_send()

    pl.when((core == 1) & jnp.logical_not(bypassed))(functools.partial(relayed, 2 * DEPTH - 1))
    pl.when(bypassed)(functools.partial(relayed, 2 * DEPTH - 2))

    @pl.when(is_direct)
    def _():
        part = tags.at[two(0)]
        remote(part, part, send_direct, recv_direct, me ^ 1).wait_send()
        part = packed.at[0, EARLIEST]
        remote(part, part, send_rows, recv_depth, me ^ 1).wait_send()


def write_out(mean, rarity, mean_hbm, rarity_hbm, sems):
    copies = [
        pltpu.make_async_copy(mean, mean_hbm, sems.at[0]),
        pltpu.make_async_copy(rarity, rarity_hbm, sems.at[1]),
    ]
    for copy in copies:
        copy.start()
    for copy in copies:
        copy.wait()


def shards(goal_embed, goal_bins, goal_weights):
    width = goal_embed.shape[1]
    goals = goal_embed.shape[0]
    vmem = pl.BlockSpec(memory_space=pltpu.VMEM)
    hbm = pl.BlockSpec(memory_space=pltpu.HBM)
    dma = pltpu.SemaphoreType.DMA
    shapes = (
        jax.ShapeDtypeStruct((BINS_DEV, width), jnp.float32),
        jax.ShapeDtypeStruct((1, BINS_DEV), jnp.float32),
    )
    results = pl.pallas_call(
        exchange,
        out_shape=shapes,
        in_specs=[hbm] * 3,
        out_specs=(vmem, vmem),
        scratch_shapes=[
            pltpu.VMEM((goals, width), jnp.bfloat16),
            pltpu.VMEM((1, goals), jnp.int32),
            pltpu.VMEM((1, goals), jnp.float32),
            pltpu.VMEM((CHIPS, 2 * DEPTH, 2, width), jnp.bfloat16),
            pltpu.VMEM((PLANE, 2 * DEPTH, 2, width), jnp.bfloat16),
            pltpu.VMEM((DEPTH, PLANE, 2, width), jnp.bfloat16),
            pltpu.VMEM((2 * CHIPS, 128), jnp.float32),
            pltpu.VMEM((2 * PLANE, 128), jnp.float32),
            pltpu.VMEM((2 * len(DIRECT) * PLANE, 128), jnp.float32),
            pltpu.VMEM((4 * DEPTH, 128), jnp.float32),
            pltpu.VMEM((2 * DEPTH, 128), jnp.float32),
            dma((3,)), dma(()), dma((4,)), dma((len(TIERS),)), dma(()), dma(()), dma(()), dma(()), dma(()), dma(()),
            dma(()), dma(()), dma(()),
            pltpu.SemaphoreType.REGULAR, pltpu.SemaphoreType.REGULAR,
        ],
        compiler_params=pltpu.CompilerParams(collective_id=0, has_side_effects=True, vmem_limit_bytes=4 << 20),
        name="exchange",
    )(*[
        pltpu.with_memory_space_constraint(array, pltpu.HBM)
        for array in (goal_embed, goal_bins.reshape(1, goals), goal_weights.reshape(1, goals))
    ])
    mean, rarity = pl.pallas_call(
        write_out,
        out_shape=shapes,
        in_specs=[vmem, vmem],
        out_specs=(hbm, hbm),
        scratch_shapes=[dma((2,))],
        compiler_params=pltpu.CompilerParams(vmem_limit_bytes=1 << 20),
        name="write_out",
    )(*results)
    return mean, rarity[0]


def solution(mesh):
    flat = Mesh(mesh.devices.reshape(-1), (AXIS,))
    return jax.shard_map(
        shards, mesh=flat, in_specs=(P(AXIS, None), P(AXIS), P(AXIS)),
        out_specs=(P(AXIS, None), P(AXIS)), check_vma=False,
    )
```
